128 devices in a mesh: shard: 8 (over x, core), member: 16 (over z, y).
Axes of the slice: x: 4, y: 4, z: 4, core: 2. Of those that a mesh axis runs over, the one named last changes fastest.
Arguments:
- embeddings: float32 [32768, 768], P(('shard', 'member')), may hold values from -1200 to 1200
- clusters: int32 [32768], P(('shard', 'member')), may hold values from 0 to 255, as said below
- row_ids: int32 [32768], P(('shard', 'member')), may hold values from 0 to 32767, each once
- owner_map: int32 [256], replicated, may hold values from 0 to 127, as said below
Outputs:
- centroids: float32 [256, 768], P(('shard', 'member'))
- earlier_max: float32 [32768], P(('shard', 'member'))
The draws below stay inside these ranges and needn't reach their ends.
Inputs may be any that keep to these rules, and one draw needn't show every extreme that they name: Of the rows of one device, at most 6 lie in clusters of any one owner; one owner index, the same for all devices, gets exactly 6 rows from every device. `owner_map`: every owner index owns exactly 2 clusters.
All inputs are finite; a program needn't handle non-finite values.
Results may differ from the reference program's by a relative error of at most 0.00042.
Values may be sent and summed in bfloat16 or wider, within the bound.
No kernel may reach another device: no remote copies, remote signals or barrier semaphores. Data moves between devices by JAX's collectives and lax.ppermute only.
A program may use at most 64 MiB of HBM per device.

```python
import math
import jax
import jax.numpy as jnp
from jax import lax

D = 768
ROW_DEV = 256
CL_OWN = 2
CLUSTERS = 256
CAP = 6
ROWS = 32768


subgroups = 16


def owner_table(key):
    shuffled = jax.random.permutation(jax.random.fold_in(key, 11), CLUSTERS).astype(jnp.int32)
    return ((shuffled // CL_OWN).astype(jnp.int32), shuffled)


def draw_owner_map(key, part):
    return owner_table(key)[0]


def draw_clusters(key, part):
    owners, shuffled = owner_table(key)
    inverse = jnp.argsort(shuffled).astype(jnp.int32)
    owner_count = CLUSTERS // CL_OWN
    blocks = ROWS // ROW_DEV
    slots = owner_count * CAP
    busiest = jax.random.randint(jax.random.fold_in(key, 12), (), 0, owner_count)
    random_bits = jax.random.randint(jax.random.fold_in(key, 13), (blocks, slots), 0, 1 << 18)
    slot_owner = jnp.arange(slots, dtype=jnp.int32) // CAP
    priority = random_bits * slots + jnp.arange(slots, dtype=jnp.int32)[None, :]
    priority = jnp.where(slot_owner[None, :] == busiest, priority - (1 << 30), priority)
    picked = jnp.argsort(priority, axis=1)[:, :ROW_DEV]
    chosen_owner = picked // CAP
    order_bits = jax.random.randint(jax.random.fold_in(key, 14), (blocks, ROW_DEV), 0, 1 << 18)
    shuffle = jnp.argsort(order_bits * ROW_DEV + jnp.arange(ROW_DEV, dtype=jnp.int32)[None, :], axis=1)
    row_owner = jnp.take_along_axis(chosen_owner, shuffle, axis=1)
    local_rank = jax.random.randint(jax.random.fold_in(key, 15), (blocks, ROW_DEV), 0, CL_OWN)
    return inverse[row_owner * CL_OWN + local_rank].reshape(ROWS).astype(jnp.int32)


def draw_embeddings(key, part):
    cluster_rows = draw_clusters(key, part)
    subgroup = jax.random.randint(jax.random.fold_in(key, 21), (ROWS,), 0, subgroups)
    centres = jax.random.truncated_normal(jax.random.fold_in(key, 22), -4.0, 4.0, (CLUSTERS, D), jnp.float32)
    duplicates = jax.random.truncated_normal(jax.random.fold_in(key, 23), -4.0, 4.0, (CLUSTERS * subgroups, D), jnp.float32)
    spread = jnp.exp(jax.random.uniform(jax.random.fold_in(key, 24), (ROWS,), jnp.float32, math.log(0.3), math.log(1.5)))
    scaling = jnp.exp(jax.random.uniform(jax.random.fold_in(key, 25), (ROWS,), jnp.float32, 0.0, math.log(10.0)))
    columns = jnp.arange(D, dtype=jnp.float32) / max(D - 1, 1)
    jitter = jax.random.truncated_normal(jax.random.fold_in(key, 26), -4.0, 4.0, (ROWS, D), jnp.float32)
    column_scale = 3.0 ** columns
    mixture = 0.7 * centres[cluster_rows] + duplicates[cluster_rows * subgroups + subgroup] + spread[:, None] * jitter
    return mixture * column_scale[None, :] * scaling[:, None]


def setup_inputs(seed: int = 0) -> dict:
    splits = jax.random.split(jax.random.key(seed), 5)
    embeddings = draw_embeddings(jax.random.fold_in(splits[4], 71), 0)
    clusters = draw_clusters(jax.random.fold_in(splits[4], 71), 0)
    row_ids = jax.random.permutation(splits[2], ROWS).astype(jnp.int32)
    owner_map = draw_owner_map(jax.random.fold_in(splits[4], 71), 0)
    return {"embeddings": embeddings, "clusters": clusters, "row_ids": row_ids, "owner_map": owner_map}


def reference(embeddings, clusters, row_ids, owner_map):
    cluster_count = owner_map.shape[0]
    row_count = embeddings.shape[0]
    owner_count = cluster_count // CL_OWN
    window = 3 * ROW_DEV
    positions = jnp.arange(cluster_count, dtype=jnp.int32)
    same_owner = owner_map[None, :] == owner_map[:, None]
    earlier_cluster = positions[None, :] < positions[:, None]
    owner_rank = lax.optimization_barrier(jnp.sum((same_owner & earlier_cluster).astype(jnp.int32), axis=1)).astype(jnp.int32)
    place = (owner_map * CL_OWN + owner_rank).astype(jnp.int32)
    cluster_sums = jax.ops.segment_sum(embeddings, place[clusters], num_segments=cluster_count)
    centroids = cluster_sums * lax.rsqrt(lax.optimization_barrier(jnp.mean(cluster_sums * cluster_sums, axis=1, keepdims=True)) + 1e-06)
    unit_vectors = (embeddings * lax.rsqrt(lax.optimization_barrier(jnp.sum(embeddings * embeddings, axis=1, keepdims=True)) + 1e-06)).astype(jnp.bfloat16)
    unit_keys = unit_vectors.astype(jnp.float32)
    row_owner = owner_map[clusters].astype(jnp.int32)
    order = jnp.argsort(row_owner, stable=True).astype(jnp.int32)
    sorted_owner = row_owner[order]
    owner_index = jnp.arange(owner_count, dtype=jnp.int32)
    starts = lax.optimization_barrier(jnp.sum((row_owner[None, :] < owner_index[:, None]).astype(jnp.int32), axis=1)).astype(jnp.int32)
    padded_keys = jnp.concatenate([unit_keys[order], jnp.zeros((window, unit_keys.shape[1]), jnp.float32)], axis=0)
    padded_groups = jnp.concatenate([clusters[order], jnp.full((window,), -1, jnp.int32)], axis=0)
    padded_ids = jnp.concatenate([row_ids[order], jnp.full((window,), -1, jnp.int32)], axis=0)

    def owner_max(start):
        keys = lax.dynamic_slice_in_dim(padded_keys, start, window, 0)
        groups = lax.dynamic_slice_in_dim(padded_groups, start, window, 0)
        ids = lax.dynamic_slice_in_dim(padded_ids, start, window, 0)
        scores = lax.dot_general(keys, keys, (((1,), (1,)), ((), ())), precision=lax.Precision.HIGHEST, preferred_element_type=jnp.float32)
        allowed = (groups[:, None] == groups[None, :]) & (ids[None, :] < ids[:, None])
        return lax.optimization_barrier(jnp.max(jnp.where(allowed, scores, -1.0), axis=1))
    owner_results = lax.map(owner_max, starts)
    sorted_positions = jnp.arange(row_count, dtype=jnp.int32)
    sorted_values = owner_results[sorted_owner, sorted_positions - starts[sorted_owner]]
    earlier_max = jnp.zeros((row_count,), jnp.float32).at[order].set(sorted_values)
    return (centroids, earlier_max)
```

```python
import jax
import jax.numpy as jnp
from jax import lax
from jax.experimental import pallas as pl
from jax.experimental.pallas import tpu as pltpu
from jax.sharding import PartitionSpec as P

epsilon = 1e-06
axes = ("shard", "member")
sent_rows = 8
lanes = 128
id_base = 256
id_range = 32768
f32 = jnp.float32
bf16 = jnp.bfloat16
i32 = jnp.int32


def iota(shape, dim):
    return lax.broadcasted_iota(i32, shape, dim)


def dot(a, b, contract=((1,), (0,))):
    return lax.dot_general(a, b, (contract, ((), ())), preferred_element_type=f32)


def one_hot(mask):
    return jnp.where(mask, 1.0, 0.0).astype(bf16)


def column(row):
    n = row.shape[1]
    diagonal = iota((n, n), 0) == iota((n, n), 1)
    spread = jnp.where(diagonal, row.astype(f32), 0.0).astype(bf16)
    return dot(spread, jnp.ones((n, n), bf16))


def earlier_equal(row):
    n = row.shape[1]
    before = iota((n, n), 0) < iota((n, n), 1)
    hits = before & (column(row) == row.astype(f32))
    return jnp.sum(jnp.where(hits, 1.0, 0.0), axis=0, keepdims=True)


def pack_kernel(rows_ref, clusters_ref, ids_ref, owners_ref, sent_ref, route_ref):
    rows = rows_ref[...]
    clusters = clusters_ref[...]
    ids = ids_ref[...]
    owner_map = owners_ref[...]
    row_count, width = rows.shape
    slot_count = sent_ref.shape[0]
    cluster_count = owner_map.shape[1]

    rank_map = earlier_equal(owner_map)
    sub = iota((8, cluster_count), 0)
    table = jnp.where(sub == 0, owner_map.astype(f32), jnp.where(sub == 1, rank_map, 0.0))
    cluster_hot = one_hot(iota((cluster_count, row_count), 0) == clusters)
    found = dot(table.astype(bf16), cluster_hot)
    owner = found[0:1].astype(i32)
    rank = found[1:2].astype(i32)
    slot = earlier_equal(owner).astype(i32)
    target = owner * sent_rows + slot
    spill = owner * sent_rows + (sent_rows - 2) + rank

    power = jnp.sum(rows * rows, axis=1, keepdims=True) + epsilon
    inverse = lax.rsqrt(power)
    unit = (rows * inverse).astype(bf16)
    norm = (power * inverse).astype(bf16)
    residual = (rows - unit.astype(f32) * norm.astype(f32)).astype(bf16)

    high = ids // id_base
    sub = iota((lanes, row_count), 0)
    notes = jnp.where(sub == 0, high, 0)
    notes = jnp.where(sub == 1, ids - high * id_base, notes)
    notes = jnp.where(sub == 2, rank + 1, notes).astype(f32).astype(bf16)
    norm_lane = jnp.where(iota((row_count, lanes), 1) == 3, norm.astype(f32), 0.0).astype(bf16)

    place = iota((slot_count, row_count), 0)
    take = one_hot(place == target)
    take_spill = one_hot(place == spill)
    sent_ref[:, :width] = (dot(take, unit) + dot(take_spill, residual)).astype(bf16)
    sent_ref[:, width:] = (dot(take, notes, ((1,), (1,))) + dot(take, norm_lane)).astype(bf16)
    sub = iota(route_ref.shape, 0)
    route_ref[...] = jnp.where(sub == 0, owner, slot)


def score_kernel(got_ref, sums_ref, best_ref, *, block):
    slot_count = got_ref.shape[0]
    width = got_ref.shape[1] - lanes
    notes = got_ref[:, width:]

    sub = iota((8, lanes), 0)
    lane = iota((8, lanes), 1)
    pick = jnp.where((sub == 0) & (lane == 0), float(id_base), 0.0)
    pick = jnp.where((sub == 0) & (lane == 1), 1.0, pick)
    pick = jnp.where((sub == 0) & (lane == 2), float(id_range), pick)
    pick = jnp.where((sub == 1) & (lane == 2), 1.0, pick)
    pick = jnp.where((sub == 2) & (lane == 3), 1.0, pick).astype(bf16)
    wide = dot(pick, notes, ((1,), (1,)))
    key_row = wide[0:1]
    rank_row = wide[1:2]
    norm_row = wide[2:3]
    base_row = rank_row * float(id_range)
    lane = iota((lanes, lanes), 0)
    spread = jnp.where(lane == 0, float(id_base), 0.0)
    spread = jnp.where(lane == 1, 1.0, spread)
    spread = jnp.where(lane == 2, float(id_range), spread).astype(bf16)
    key_col = dot(notes, spread)

    sub = iota((8, slot_count), 0)
    within = iota((8, slot_count), 1) % sent_rows
    weight = jnp.where(rank_row == (sub + 1).astype(f32), norm_row, 0.0)
    weight = weight + jnp.where(within == sub + (sent_rows - 2), 1.0, 0.0)
    sums = dot(weight.astype(bf16), got_ref[:, :width])
    sums = sums[0 : sums_ref.shape[0]]
    scale = lax.rsqrt(jnp.mean(sums * sums, axis=1, keepdims=True) + epsilon)
    sums_ref[...] = sums * scale

    keys = got_ref[:, :width]
    for start in range(0, slot_count, block):
        stop = start + block
        scores = dot(keys, got_ref[start:stop, :width], ((1,), (1,)))
        low = base_row[:, start:stop]
        high = key_row[:, start:stop]
        other = jnp.concatenate([key_col] * (block // lanes), axis=1)
        allowed = (other >= low) & (other < high)
        best = jnp.max(jnp.where(allowed, scores, -1.0), axis=0, keepdims=True)
        peers = block // sent_rows
        mine = iota((peers, block), 1) // sent_rows == iota((peers, block), 0)
        spread_best = jnp.where(mine, best, 0.0)
        lane_of = one_hot(iota((block, lanes), 0) % sent_rows == iota((block, lanes), 1))
        best_ref[start // sent_rows : stop // sent_rows, :] = exact_dot(spread_best, lane_of)


def exact_dot(values, hot, contract=((1,), (0,))):
    first = values.astype(bf16)
    rest = values - first.astype(f32)
    second = rest.astype(bf16)
    third = (rest - second.astype(f32)).astype(bf16)
    return dot(first, hot, contract) + dot(second, hot, contract) + dot(third, hot, contract)


def unpack_kernel(back_ref, route_ref, out_ref):
    owner = route_ref[0:1, :]
    slot = route_ref[1:2, :]
    back = back_ref[...]
    row_count = owner.shape[1]
    hot = one_hot(iota((back.shape[0], row_count), 0) == owner)
    found = exact_dot(back, hot, ((0,), (0,)))[0:8]
    mine = iota((8, row_count), 0) == slot
    out_ref[...] = jnp.sum(jnp.where(mine, found, 0.0), axis=0, keepdims=True)


def shards(embeddings, clusters, row_ids, owner_map):
    owners = lax.axis_size("shard") * lax.axis_size("member")
    local_rows, width = embeddings.shape
    cluster_count = owner_map.shape[0]
    per_owner = cluster_count // owners
    slots = owners * sent_rows
    packed, route = pl.pallas_call(
        pack_kernel,
        out_shape=(
            jax.ShapeDtypeStruct((slots, width + lanes), bf16),
            jax.ShapeDtypeStruct((8, local_rows), i32),
        ),
        name="pack",
    )(
        embeddings,
        clusters.reshape(1, local_rows),
        row_ids.reshape(1, local_rows),
        owner_map.reshape(1, cluster_count),
    )
    received = lax.all_to_all(packed, axes, split_axis=0, concat_axis=0, tiled=True)
    centroids, best = pl.pallas_call(
        lambda *refs: score_kernel(*refs, block=256),
        out_shape=(
            jax.ShapeDtypeStruct((per_owner, width), f32),
            jax.ShapeDtypeStruct((owners, lanes), f32),
        ),
        name="score",
    )(received)
    returned = lax.all_to_all(
        best.reshape(owners, 1, lanes), axes, split_axis=0, concat_axis=0, tiled=True
    )
    earlier_max = pl.pallas_call(
        unpack_kernel,
        out_shape=jax.ShapeDtypeStruct((1, local_rows), f32),
        name="unpack",
    )(returned.reshape(owners, lanes), route)
    return (centroids, earlier_max.reshape(local_rows))


def solution(mesh):
    placed = (P(axes, None), P(axes), P(axes), P())
    return jax.shard_map(
        shards,
        mesh=mesh,
        in_specs=placed,
        out_specs=(P(axes, None), P(axes)),
        check_vma=False,
    )
```

```python
import jax
import jax.numpy as jnp
from jax import lax
from jax.experimental import pallas as pl
from jax.experimental.pallas import tpu as pltpu
from jax.sharding import PartitionSpec as P

epsilon = 1e-06
axes = ("shard", "member")
pairs = 3
lanes = 128
id_base = 256
id_range = 32768
f32 = jnp.float32
bf16 = jnp.bfloat16
i32 = jnp.int32
params = pltpu.CompilerParams(vmem_limit_bytes=24 << 20)


def iota(shape, dim):
    return lax.broadcasted_iota(i32, shape, dim)


def dot(a, b, contract=((1,), (0,))):
    return lax.dot_general(a, b, (contract, ((), ())), preferred_element_type=f32)


def one_hot(mask):
    return jnp.where(mask, 1.0, 0.0).astype(bf16)


def count(mask):
    return jnp.sum(jnp.where(mask, 1.0, 0.0), axis=0, keepdims=True)


def pack_kernel(
    rows_hbm,
    clusters_hbm,
    ids_hbm,
    owners_hbm,
    sent_ref,
    route_ref,
    rows_ref,
    clusters_ref,
    ids_ref,
    owners_ref,
    sems,
):
    index_copies = (
        pltpu.make_async_copy(owners_hbm, owners_ref, sems.at[0]),
        pltpu.make_async_copy(clusters_hbm, clusters_ref, sems.at[1]),
        pltpu.make_async_copy(ids_hbm, ids_ref, sems.at[2]),
    )
    copy = pltpu.make_async_copy(rows_hbm, rows_ref, sems.at[3])
    for index_copy in index_copies:
        index_copy.start()
    copy.start()
    for index_copy in index_copies:
        index_copy.wait()
    clusters = clusters_ref[...]
    ids = ids_ref[...]
    owner_map = owners_ref[...].astype(f32)
    row_count, width = rows_ref.shape
    owners = sent_ref.shape[0]
    cluster_count = owner_map.shape[1]

    square = (cluster_count, cluster_count)
    diagonal = iota(square, 0) == iota(square, 1)
    before = iota(square, 0) < iota(square, 1)
    spread = jnp.where(diagonal, owner_map, 0.0).astype(bf16)
    map_col = dot(spread, jnp.ones(square, bf16))
    rank_map = count(before & (map_col == owner_map))
    sub = iota((8, cluster_count), 0)
    table = jnp.where(sub == 0, owner_map, jnp.where(sub == 1, rank_map, 0.0)).astype(bf16)
    cluster_hot = one_hot(iota((cluster_count, row_count), 0) == clusters)
    found = dot(table, cluster_hot)
    owner_col = dot(cluster_hot, map_col[:, :row_count].astype(bf16), ((0,), (0,)))
    slot = count(before & (owner_col == found[0:1])).astype(i32)
    owner = found[0:1].astype(i32)
    rank = found[1:2].astype(i32)
    pair = slot // 2
    target = owner * 2 + slot % 2

    copy.wait()
    rows = rows_ref[...]
    power = jnp.sum(rows * rows, axis=1, keepdims=True) + epsilon
    inverse = lax.rsqrt(power)
    unit = (rows * inverse).astype(bf16)
    norm = (power * inverse).astype(bf16).astype(f32)
    residual = (rows - unit.astype(f32) * norm).astype(bf16)
    norm_row = jnp.sum(jnp.where(diagonal, norm, 0.0), axis=0, keepdims=True)

    high = ids // id_base
    lane = iota((lanes, row_count), 0)
    field = jnp.where(lane // 4 == pair, lane % 4, -1)
    notes = jnp.where(field == 0, high.astype(f32), 0.0)
    notes = jnp.where(field == 1, (ids - high * id_base).astype(f32), notes)
    notes = jnp.where(field == 2, (rank + 1).astype(f32), notes)
    notes = jnp.where(field == 3, norm_row, notes).astype(bf16)

    place = iota((2 * owners, row_count), 0)
    for p in range(pairs):
        take = one_hot(place == jnp.where(pair == p, target, -1))
        part = dot(take, unit).astype(bf16).reshape(owners, 2, width)
        sent_ref[:, :, p * width : (p + 1) * width] = part
    take = one_hot(place == owner * 2 + rank)
    part = dot(take, residual).astype(bf16).reshape(owners, 2, width)
    sent_ref[:, :, pairs * width : (pairs + 1) * width] = part
    take = one_hot(place == target)
    part = dot(take, notes, ((1,), (1,))).astype(bf16).reshape(owners, 2, lanes)
    sent_ref[:, :, (pairs + 1) * width :] = part
    sub = iota(route_ref.shape, 0)
    route_ref[...] = jnp.where(sub == 0, target, pair)


def score_kernel(got_ref, sums_ref, best_ref):
    owners = got_ref.shape[0]
    width = (got_ref.shape[2] - lanes) // (pairs + 1)
    block = 2 * owners
    notes = got_ref[:, :, (pairs + 1) * width :].reshape(block, lanes)
    keys = []
    for p in range(pairs):
        keys.append(got_ref[:, :, p * width : (p + 1) * width].reshape(block, width))
    residual = got_ref[:, :, pairs * width : (pairs + 1) * width].reshape(block, width)

    sub = iota((8 * pairs, lanes), 0)
    field = iota((8 * pairs, lanes), 1) - 4 * (sub // 8)
    kind = sub % 8
    pick = jnp.where((kind == 0) & (field == 0), float(id_base), 0.0)
    pick = jnp.where((kind == 0) & (field == 1), 1.0, pick)
    pick = jnp.where((kind == 0) & (field == 2), float(id_range), pick)
    pick = jnp.where((kind == 1) & (field == 2), 1.0, pick)
    pick = jnp.where((kind == 2) & (field == 3), 1.0, pick).astype(bf16)
    wide = dot(pick, notes, ((1,), (1,)))
    field = iota((lanes, pairs * lanes), 0) - 4 * (iota((lanes, pairs * lanes), 1) // lanes)
    spread = jnp.where(field == 0, float(id_base), 0.0)
    spread = jnp.where(field == 1, 1.0, spread)
    spread = jnp.where(field == 2, float(id_range), spread).astype(bf16)
    key_col = dot(notes, spread)

    sub = iota((8, block), 0)
    sums = dot(one_hot(iota((8, block), 1) % 2 == sub), residual)
    for p in range(pairs):
        ranks = wide[8 * p + 1 : 8 * p + 2]
        norms = wide[8 * p + 2 : 8 * p + 3]
        weight = jnp.where(ranks == (sub + 1).astype(f32), norms, 0.0)
        sums = sums + dot(weight.astype(bf16), keys[p])
    sums = sums[0 : sums_ref.shape[0]]
    scale = lax.rsqrt(jnp.mean(sums * sums, axis=1, keepdims=True) + epsilon)
    sums_ref[...] = sums * scale

    bests = jnp.full((lanes, block), -1.0, f32)
    for q in range(pairs):
        high = wide[8 * q : 8 * q + 1]
        low = wide[8 * q + 1 : 8 * q + 2] * float(id_range)
        best = jnp.full((1, block), -1.0, f32)
        for p in range(pairs):
            scores = dot(keys[p], keys[q], ((1,), (1,)))
            other = key_col[:, p * lanes : (p + 1) * lanes]
            other = jnp.concatenate([other] * (block // lanes), axis=1)
            allowed = (other >= low) & (other < high)
            found = jnp.max(jnp.where(allowed, scores, -1.0), axis=0, keepdims=True)
            best = jnp.maximum(best, found)
        bests = jnp.where(iota((lanes, block), 0) == q, best, bests)
    best_ref[...] = bests.T


def exact_dot(values, hot, contract=((1,), (0,))):
    first = values.astype(bf16)
    rest = values - first.astype(f32)
    second = rest.astype(bf16)
    third = (rest - second.astype(f32)).astype(bf16)
    return dot(first, hot, contract) + dot(second, hot, contract) + dot(third, hot, contract)


def unpack_kernel(back_ref, route_ref, out_ref):
    target = route_ref[0:1, :]
    pair = route_ref[1:2, :]
    back = back_ref[...]
    row_count = target.shape[1]
    hot = one_hot(iota((back.shape[0], row_count), 0) == target)
    found = exact_dot(back, hot, ((0,), (0,)))[0:8]
    mine = iota((8, row_count), 0) == pair
    out_ref[...] = jnp.sum(jnp.where(mine, found, 0.0), axis=0, keepdims=True)


def shards(embeddings, clusters, row_ids, owner_map):
    owners = lax.axis_size("shard") * lax.axis_size("member")
    local_rows, width = embeddings.shape
    cluster_count = owner_map.shape[0]
    per_owner = cluster_count // owners
    hbm = pl.BlockSpec(memory_space=pltpu.HBM)
    packed, route = pl.pallas_call(
        pack_kernel,
        in_specs=[hbm] * 4,
        out_shape=(
            jax.ShapeDtypeStruct((owners, 2, (pairs + 1) * width + lanes), bf16),
            jax.ShapeDtypeStruct((8, local_rows), i32),
        ),
        scratch_shapes=[
            pltpu.VMEM((local_rows, width), f32),
            pltpu.VMEM((1, local_rows), i32),
            pltpu.VMEM((1, local_rows), i32),
            pltpu.VMEM((1, cluster_count), i32),
            pltpu.SemaphoreType.DMA((4,)),
        ],
        compiler_params=params,
        name="pack",
    )(
        *[
            pltpu.with_memory_space_constraint(x, pltpu.HBM)
            for x in (
                embeddings,
                clusters.reshape(1, local_rows),
                row_ids.reshape(1, local_rows),
                owner_map.reshape(1, cluster_count),
            )
        ]
    )
    received = lax.all_to_all(packed, axes, split_axis=0, concat_axis=0, tiled=True)
    centroids, best = pl.pallas_call(
        score_kernel,
        out_shape=(
            jax.ShapeDtypeStruct((per_owner, width), f32),
            jax.ShapeDtypeStruct((2 * owners, lanes), f32),
        ),
        compiler_params=params,
        name="score",
    )(received)
    returned = lax.all_to_all(
        best.reshape(owners, 2, lanes), axes, split_axis=0, concat_axis=0, tiled=True
    )
    earlier_max = pl.pallas_call(
        unpack_kernel,
        out_shape=jax.ShapeDtypeStruct((1, local_rows), f32),
        compiler_params=params,
        name="unpack",
    )(returned.reshape(2 * owners, lanes), route)
    return (centroids, earlier_max.reshape(local_rows))


def solution(mesh):
    placed = (P(axes, None), P(axes), P(axes), P())
    return jax.shard_map(
        shards,
        mesh=mesh,
        in_specs=placed,
        out_specs=(P(axes, None), P(axes)),
        check_vma=False,
    )
```

```python
import jax
import jax.numpy as jnp
from jax import lax
from jax.experimental import pallas as pl
from jax.experimental.pallas import tpu as pltpu
from jax.sharding import PartitionSpec as P

epsilon = 1e-06
axes = ("shard", "member")
pairs = 3
lanes = 128
id_base = 256
id_range = 32768
full = 32767.0
fields = 16
norm_unit = 256
norm_bytes = 6
f32 = jnp.float32
bf16 = jnp.bfloat16
i32 = jnp.int32
i16 = jnp.int16
params = pltpu.CompilerParams(vmem_limit_bytes=24 << 20)


def iota(shape, dim):
    return lax.broadcasted_iota(i32, shape, dim)


def dot(a, b, contract=((1,), (0,))):
    return lax.dot_general(a, b, (contract, ((), ())), preferred_element_type=f32)


def one_hot(mask):
    return jnp.where(mask, 1.0, 0.0).astype(bf16)


def count(mask):
    return jnp.sum(jnp.where(mask, 1.0, 0.0), axis=0, keepdims=True)


def to_bytes(values, unit, n):
    digits = []
    rest = values * (1.0 / unit)
    for _ in range(n):
        digit = jnp.floor(rest)
        digits.append(digit)
        rest = (rest - digit) * id_base
    return digits


def pack_kernel(
    rows_hbm,
    clusters_hbm,
    ids_hbm,
    owners_hbm,
    sent_ref,
    route_ref,
    rows_ref,
    clusters_ref,
    ids_ref,
    owners_ref,
    sems,
):
    index_copies = (
        pltpu.make_async_copy(owners_hbm, owners_ref, sems.at[0]),
        pltpu.make_async_copy(clusters_hbm, clusters_ref, sems.at[1]),
        pltpu.make_async_copy(ids_hbm, ids_ref, sems.at[2]),
    )
    copy = pltpu.make_async_copy(rows_hbm, rows_ref, sems.at[3])
    for index_copy in index_copies:
        index_copy.start()
    copy.start()
    for index_copy in index_copies:
        index_copy.wait()
    clusters = clusters_ref[...]
    ids = ids_ref[...]
    owner_map = owners_ref[...].astype(f32)
    row_count, width = rows_ref.shape
    owners = sent_ref.shape[0]
    cluster_count = owner_map.shape[1]

    square = (cluster_count, cluster_count)
    diagonal = iota(square, 0) == iota(square, 1)
    before = iota(square, 0) < iota(square, 1)
    spread = jnp.where(diagonal, owner_map, 0.0).astype(bf16)
    map_col = dot(spread, jnp.ones(square, bf16))
    rank_map = count(before & (map_col == owner_map))
    sub = iota((8, cluster_count), 0)
    table = jnp.where(sub == 0, owner_map, jnp.where(sub == 1, rank_map, 0.0)).astype(bf16)
    cluster_hot = one_hot(iota((cluster_count, row_count), 0) == clusters)
    found = dot(table, cluster_hot)
    owner_col = dot(cluster_hot, map_col[:, :row_count].astype(bf16), ((0,), (0,)))
    slot = count(before & (owner_col == found[0:1])).astype(i32)
    owner = found[0:1].astype(i32)
    rank = found[1:2].astype(i32)
    pair = slot // 2
    target = owner * 2 + slot % 2

    copy.wait()
    rows = rows_ref[...]
    power = jnp.sum(rows * rows, axis=1, keepdims=True) + epsilon
    inverse = lax.rsqrt(power)
    norm = power * inverse
    largest = jnp.max(jnp.abs(rows), axis=1, keepdims=True) * inverse
    step = jnp.clip(jnp.ceil(largest * full), 1.0, full)
    codes = jnp.floor(rows * (inverse * (full * full / step)) + 0.5)
    codes = jnp.clip(codes, -full, full)
    upper = jnp.floor(codes * (1.0 / id_base)) * id_base
    halves = jnp.concatenate([upper.astype(bf16), (codes - upper).astype(bf16)], axis=0)
    norm_row = jnp.sum(jnp.where(diagonal, norm, 0.0), axis=0, keepdims=True)
    step_row = jnp.sum(jnp.where(diagonal, step, 0.0), axis=0, keepdims=True)

    values = to_bytes(ids.astype(f32), id_base, 2)
    values = values + [(rank + 1).astype(f32)]
    values = values + to_bytes(step_row, id_base, 2)
    values = values + to_bytes(norm_row, norm_unit, norm_bytes)
    lane = iota((lanes, row_count), 0)
    field = jnp.where(lane // fields == pair, lane % fields, -1)
    notes = jnp.zeros((lanes, row_count), f32)
    for k, value in enumerate(values):
        notes = jnp.where(field == k, value, notes)
    notes = notes.astype(bf16)

    place = iota((2 * owners, row_count), 0)
    for p in range(pairs):
        take = one_hot(place == jnp.where(pair == p, target, -1))
        part = dot(jnp.concatenate([take, take], axis=1), halves)
        part = part.astype(i32).astype(i16).reshape(owners, 2, width)
        sent_ref[:, :, p * width : (p + 1) * width] = part
    take = one_hot(place == target)
    part = dot(take, notes, ((1,), (1,)))
    part = part.astype(i32).astype(i16).reshape(owners, 2, lanes)
    sent_ref[:, :, pairs * width :] = part
    sub = iota(route_ref.shape, 0)
    route_ref[...] = jnp.where(sub == 0, target, pair)


def score_kernel(got_ref, sums_ref, best_ref):
    owners = got_ref.shape[0]
    width = (got_ref.shape[2] - lanes) // pairs
    block = 2 * owners
    notes = got_ref[:, :, pairs * width :].reshape(block, lanes)
    notes = notes.astype(i32).astype(f32).astype(bf16)

    sub = iota((8 * pairs, lanes), 0)
    field = iota((8 * pairs, lanes), 1) - fields * (sub // 8)
    kind = sub % 8
    pick = jnp.where((kind == 0) & (field == 0), float(id_base), 0.0)
    pick = jnp.where((kind == 0) & (field == 1), 1.0, pick)
    pick = jnp.where((kind == 0) & (field == 2), float(id_range), pick)
    pick = jnp.where((kind == 1) & (field == 2), 1.0, pick)
    for k in range(norm_bytes):
        weight = float(norm_unit) / float(id_base) ** k
        pick = jnp.where((kind == 2) & (field == 5 + k), weight, pick)
    wide = dot(pick.astype(bf16), notes, ((1,), (1,)))
    shape = (lanes, 2 * pairs * lanes)
    column = iota(shape, 1) // lanes
    field = iota(shape, 0) - fields * (column % pairs)
    keyed = column < pairs
    spread = jnp.where(field == jnp.where(keyed, 0, 3), float(id_base), 0.0)
    spread = jnp.where(field == jnp.where(keyed, 1, 4), 1.0, spread)
    spread = jnp.where(keyed & (field == 2), float(id_range), spread).astype(bf16)
    tall = dot(notes, spread)
    key_col = tall[:, : pairs * lanes]

    sub = iota((8, block), 0)
    keys = []
    sums = jnp.zeros((8, width), f32)
    for p in range(pairs):
        codes = got_ref[:, :, p * width : (p + 1) * width].reshape(block, width)
        step = tall[:, (pairs + p) * lanes : (pairs + p + 1) * lanes] * (1.0 / (full * full))
        step = jnp.concatenate([step] * (width // lanes), axis=1)
        exact = codes.astype(i32).astype(f32) * step
        unit = exact.astype(bf16)
        rest = (exact - unit.astype(f32)).astype(bf16)
        keys.append(unit)
        ranks = wide[8 * p + 1 : 8 * p + 2]
        norms = wide[8 * p + 2 : 8 * p + 3]
        coarse = norms.astype(bf16).astype(f32)
        weight = jnp.where(sub < 2, coarse, norms - coarse)
        weight = jnp.where(ranks == (sub % 2 + 1).astype(f32), weight, 0.0)
        weight = jnp.where(sub < 4, weight, 0.0).astype(bf16)
        sums = sums + dot(weight, unit) + dot(weight, rest)
    owned = sums_ref.shape[0]
    sums = sums[0:owned] + sums[owned : 2 * owned]
    scale = lax.rsqrt(jnp.mean(sums * sums, axis=1, keepdims=True) + epsilon)
    sums_ref[...] = sums * scale

    bests = jnp.full((lanes, block), -1.0, f32)
    for q in range(pairs):
        high = wide[8 * q : 8 * q + 1]
        low = wide[8 * q + 1 : 8 * q + 2] * float(id_range)
        best = jnp.full((1, block), -1.0, f32)
        for p in range(pairs):
            scores = dot(keys[p], keys[q], ((1,), (1,)))
            other = key_col[:, p * lanes : (p + 1) * lanes]
            other = jnp.concatenate([other] * (block // lanes), axis=1)
            allowed = (other >= low) & (other < high)
            found = jnp.max(jnp.where(allowed, scores, -1.0), axis=0, keepdims=True)
            best = jnp.maximum(best, found)
        bests = jnp.where(iota((lanes, block), 0) == q, best, bests)
    best_ref[...] = bests.T


def exact_dot(values, hot, contract=((1,), (0,))):
    first = values.astype(bf16)
    rest = values - first.astype(f32)
    second = rest.astype(bf16)
    third = (rest - second.astype(f32)).astype(bf16)
    return dot(first, hot, contract) + dot(second, hot, contract) + dot(third, hot, contract)


def unpack_kernel(back_ref, route_ref, out_ref):
    target = route_ref[0:1, :]
    pair = route_ref[1:2, :]
    back = back_ref[...]
    row_count = target.shape[1]
    hot = one_hot(iota((back.shape[0], row_count), 0) == target)
    found = exact_dot(back, hot, ((0,), (0,)))[0:8]
    mine = iota((8, row_count), 0) == pair
    out_ref[...] = jnp.sum(jnp.where(mine, found, 0.0), axis=0, keepdims=True)


def shards(embeddings, clusters, row_ids, owner_map):
    owners = lax.axis_size("shard") * lax.axis_size("member")
    local_rows, width = embeddings.shape
    cluster_count = owner_map.shape[0]
    per_owner = cluster_count // owners
    hbm = pl.BlockSpec(memory_space=pltpu.HBM)
    packed, route = pl.pallas_call(
        pack_kernel,
        in_specs=[hbm] * 4,
        out_shape=(
            jax.ShapeDtypeStruct((owners, 2, pairs * width + lanes), i16),
            jax.ShapeDtypeStruct((8, local_rows), i32),
        ),
        scratch_shapes=[
            pltpu.VMEM((local_rows, width), f32),
            pltpu.VMEM((1, local_rows), i32),
            pltpu.VMEM((1, local_rows), i32),
            pltpu.VMEM((1, cluster_count), i32),
            pltpu.SemaphoreType.DMA((4,)),
        ],
        compiler_params=params,
        name="pack",
    )(
        *[
            pltpu.with_memory_space_constraint(x, pltpu.HBM)
            for x in (
                embeddings,
                clusters.reshape(1, local_rows),
                row_ids.reshape(1, local_rows),
                owner_map.reshape(1, cluster_count),
            )
        ]
    )
    received = lax.all_to_all(packed, axes, split_axis=0, concat_axis=0, tiled=True)
    centroids, best = pl.pallas_call(
        score_kernel,
        out_shape=(
            jax.ShapeDtypeStruct((per_owner, width), f32),
            jax.ShapeDtypeStruct((2 * owners, lanes), f32),
        ),
        compiler_params=params,
        name="score",
    )(received)
    returned = lax.all_to_all(
        best.reshape(owners, 2, lanes), axes, split_axis=0, concat_axis=0, tiled=True
    )
    earlier_max = pl.pallas_call(
        unpack_kernel,
        out_shape=jax.ShapeDtypeStruct((1, local_rows), f32),
        compiler_params=params,
        name="unpack",
    )(returned.reshape(2 * owners, lanes), route)
    return (centroids, earlier_max.reshape(local_rows))


def solution(mesh):
    placed = (P(axes, None), P(axes), P(axes), P())
    return jax.shard_map(
        shards,
        mesh=mesh,
        in_specs=placed,
        out_specs=(P(axes, None), P(axes)),
        check_vma=False,
    )
```

```python
import jax
import jax.numpy as jnp
from jax import lax
from jax.experimental import pallas as pl
from jax.experimental.pallas import tpu as pltpu
from jax.sharding import PartitionSpec as P

epsilon = 1e-06
axes = ("shard", "member")
pairs = 3
lanes = 128
id_base = 256
id_range = 32768
full = 32767.0
fields = 16
norm_unit = 256
norm_bytes = 6
f32 = jnp.float32
bf16 = jnp.bfloat16
i32 = jnp.int32
i16 = jnp.int16
params = pltpu.CompilerParams(vmem_limit_bytes=24 << 20)


def iota(shape, dim):
    return lax.broadcasted_iota(i32, shape, dim)


def dot(a, b, contract=((1,), (0,))):
    return lax.dot_general(a, b, (contract, ((), ())), preferred_element_type=f32)


def one_hot(mask):
    return jnp.where(mask, 1.0, 0.0).astype(bf16)


def count(mask):
    return jnp.sum(jnp.where(mask, 1.0, 0.0), axis=0, keepdims=True)


def to_bytes(values, unit, n):
    digits = []
    rest = values * (1.0 / unit)
    for _ in range(n):
        digit = jnp.floor(rest)
        digits.append(digit)
        rest = (rest - digit) * id_base
    return digits


def pack_kernel(
    rows_hbm,
    clusters_hbm,
    ids_hbm,
    owners_hbm,
    sent_ref,
    route_ref,
    rows_ref,
    clusters_ref,
    ids_ref,
    owners_ref,
    sems,
):
    index_copies = (
        pltpu.make_async_copy(owners_hbm, owners_ref, sems.at[0]),
        pltpu.make_async_copy(clusters_hbm, clusters_ref, sems.at[1]),
        pltpu.make_async_copy(ids_hbm, ids_ref, sems.at[2]),
    )
    copy = pltpu.make_async_copy(rows_hbm, rows_ref, sems.at[3])
    for index_copy in index_copies:
        index_copy.start()
    copy.start()
    for index_copy in index_copies:
        index_copy.wait()
    clusters = clusters_ref[...]
    ids = ids_ref[...]
    owner_map = owners_ref[...].astype(f32)
    row_count, width = rows_ref.shape
    owners = sent_ref.shape[0]
    cluster_count = owner_map.shape[1]

    square = (cluster_count, cluster_count)
    diagonal = iota(square, 0) == iota(square, 1)
    before = iota(square, 0) < iota(square, 1)
    spread = jnp.where(diagonal, owner_map, 0.0).astype(bf16)
    map_col = dot(spread, jnp.ones(square, bf16))
    rank_map = count(before & (map_col == owner_map))
    sub = iota((8, cluster_count), 0)
    table = jnp.where(sub == 0, owner_map, jnp.where(sub == 1, rank_map, 0.0)).astype(bf16)
    cluster_hot = one_hot(iota((cluster_count, row_count), 0) == clusters)
    found = dot(table, cluster_hot)
    owner_col = dot(cluster_hot, map_col[:, :row_count].astype(bf16), ((0,), (0,)))
    slot = count(before & (owner_col == found[0:1])).astype(i32)
    owner = found[0:1].astype(i32)
    rank = found[1:2].astype(i32)
    pair = slot // 2
    target = owner * 2 + slot % 2

    copy.wait()
    rows = rows_ref[...]
    power = jnp.sum(rows * rows, axis=1, keepdims=True) + epsilon
    inverse = lax.rsqrt(power)
    norm = power * inverse
    largest = jnp.max(jnp.abs(rows), axis=1, keepdims=True) * inverse
    step = jnp.clip(jnp.ceil(largest * full), 1.0, full)
    codes = jnp.floor(rows * (inverse * (full * full / step)) + 0.5)
    codes = jnp.clip(codes, -full, full)
    upper = jnp.floor(codes * (1.0 / id_base)) * id_base
    halves = jnp.concatenate([upper.astype(bf16), (codes - upper).astype(bf16)], axis=0)
    norm_row = jnp.sum(jnp.where(diagonal, norm, 0.0), axis=0, keepdims=True)
    step_row = jnp.sum(jnp.where(diagonal, step, 0.0), axis=0, keepdims=True)

    values = to_bytes(ids.astype(f32), id_base, 2)
    values = values + [(rank + 1).astype(f32)]
    values = values + to_bytes(step_row, id_base, 2)
    values = values + to_bytes(norm_row, norm_unit, norm_bytes)
    lane = iota((lanes, row_count), 0)
    field = jnp.where(lane // fields == pair, lane % fields, -1)
    notes = jnp.zeros((lanes, row_count), f32)
    for k, value in enumerate(values):
        notes = jnp.where(field == k, value, notes)
    notes = notes.astype(bf16)

    place = iota((2 * owners, row_count), 0)
    for p in range(pairs):
        take = one_hot(place == jnp.where(pair == p, target, -1))
        part = dot(jnp.concatenate([take, take], axis=1), halves)
        part = part.astype(i32).astype(i16).reshape(owners, 2, width)
        sent_ref[:, :, p * width : (p + 1) * width] = part
    take = one_hot(place == target)
    part = dot(take, notes, ((1,), (1,)))
    part = part.astype(i32).astype(i16).reshape(owners, 2, lanes)
    sent_ref[:, :, pairs * width :] = part
    sub = iota(route_ref.shape, 0)
    route_ref[...] = jnp.where(sub == 0, target, pair)


def read_notes(got_ref):
    owners = got_ref.shape[0]
    notes = got_ref[:, :, got_ref.shape[2] - lanes :].reshape(2 * owners, lanes)
    return notes.astype(i32).astype(f32).astype(bf16)


def read_rows(got_ref, p, step):
    owners = got_ref.shape[0]
    width = (got_ref.shape[2] - lanes) // pairs
    codes = got_ref[:, :, p * width : (p + 1) * width].reshape(2 * owners, width)
    step = jnp.concatenate([step * (1.0 / (full * full))] * (width // lanes), axis=1)
    return codes.astype(i32).astype(f32) * step


def along_sublanes(notes, first, third):
    shape = (lanes, pairs * lanes)
    field = iota(shape, 0) - fields * (iota(shape, 1) // lanes)
    spread = jnp.where(field == first, float(id_base), 0.0)
    spread = jnp.where(field == first + 1, 1.0, spread)
    if third is not None:
        spread = jnp.where(field == third, float(id_range), spread)
    tall = dot(notes, spread.astype(bf16))
    return [tall[:, p * lanes : (p + 1) * lanes] for p in range(pairs)]


def score_kernel(got_ref, best_ref):
    block = 2 * got_ref.shape[0]
    notes = read_notes(got_ref)
    sub = iota((8 * pairs, lanes), 0)
    field = iota((8 * pairs, lanes), 1) - fields * (sub // 8)
    kind = sub % 8
    pick = jnp.where((kind == 0) & (field == 0), float(id_base), 0.0)
    pick = jnp.where((kind == 0) & (field == 1), 1.0, pick)
    pick = jnp.where((kind == 0) & (field == 2), float(id_range), pick)
    pick = jnp.where((kind == 1) & (field == 2), 1.0, pick)
    wide = dot(pick.astype(bf16), notes, ((1,), (1,)))
    key = along_sublanes(notes, 0, 2)
    step = along_sublanes(notes, 3, None)
    keys = [read_rows(got_ref, p, step[p]).astype(bf16) for p in range(pairs)]

    bests = jnp.full((lanes, block), -1.0, f32)
    for q in range(pairs):
        high = wide[8 * q : 8 * q + 1]
        low = wide[8 * q + 1 : 8 * q + 2] * float(id_range)
        best = jnp.full((1, block), -1.0, f32)
        for p in range(pairs):
            scores = dot(keys[p], keys[q], ((1,), (1,)))
            other = jnp.concatenate([key[p]] * (block // lanes), axis=1)
            allowed = (other >= low) & (other < high)
            found = jnp.max(jnp.where(allowed, scores, -1.0), axis=0, keepdims=True)
            best = jnp.maximum(best, found)
        bests = jnp.where(iota((lanes, block), 0) == q, best, bests)
    best_ref[...] = bests.T


def centre_kernel(got_ref, sums_ref):
    owned, width = sums_ref.shape
    block = 2 * got_ref.shape[0]
    notes = read_notes(got_ref)
    sub = iota((8 * pairs, lanes), 0)
    field = iota((8 * pairs, lanes), 1) - fields * (sub // 8)
    kind = sub % 8
    pick = jnp.where((kind == 1) & (field == 2), 1.0, 0.0)
    for k in range(norm_bytes):
        weight = float(norm_unit) / float(id_base) ** k
        pick = jnp.where((kind == 0) & (field == 5 + k), weight, pick)
    wide = dot(pick.astype(bf16), notes, ((1,), (1,)))
    step = along_sublanes(notes, 3, None)

    sub = iota((8, block), 0)
    sums = jnp.zeros((8, width), f32)
    for p in range(pairs):
        exact = read_rows(got_ref, p, step[p])
        unit = exact.astype(bf16)
        rest = (exact - unit.astype(f32)).astype(bf16)
        norms = wide[8 * p : 8 * p + 1]
        ranks = wide[8 * p + 1 : 8 * p + 2]
        coarse = norms.astype(bf16).astype(f32)
        weight = jnp.where(sub < owned, coarse, norms - coarse)
        weight = jnp.where(ranks == (sub % owned + 1).astype(f32), weight, 0.0)
        weight = jnp.where(sub < 2 * owned, weight, 0.0).astype(bf16)
        sums = sums + dot(weight, unit) + dot(weight, rest)
    sums = sums[0:owned] + sums[owned : 2 * owned]
    scale = lax.rsqrt(jnp.mean(sums * sums, axis=1, keepdims=True) + epsilon)
    sums_ref[...] = sums * scale


def exact_dot(values, hot, contract=((1,), (0,))):
    first = values.astype(bf16)
    rest = values - first.astype(f32)
    second = rest.astype(bf16)
    third = (rest - second.astype(f32)).astype(bf16)
    return dot(first, hot, contract) + dot(second, hot, contract) + dot(third, hot, contract)


def unpack_kernel(back_ref, route_ref, out_ref):
    target = route_ref[0:1, :]
    pair = route_ref[1:2, :]
    back = back_ref[...]
    row_count = target.shape[1]
    hot = one_hot(iota((back.shape[0], row_count), 0) == target)
    found = exact_dot(back, hot, ((0,), (0,)))[0:8]
    mine = iota((8, row_count), 0) == pair
    out_ref[...] = jnp.sum(jnp.where(mine, found, 0.0), axis=0, keepdims=True)


def shards(embeddings, clusters, row_ids, owner_map):
    owners = lax.axis_size("shard") * lax.axis_size("member")
    local_rows, width = embeddings.shape
    cluster_count = owner_map.shape[0]
    per_owner = cluster_count // owners
    hbm = pl.BlockSpec(memory_space=pltpu.HBM)
    packed, route = pl.pallas_call(
        pack_kernel,
        in_specs=[hbm] * 4,
        out_shape=(
            jax.ShapeDtypeStruct((owners, 2, pairs * width + lanes), i16),
            jax.ShapeDtypeStruct((8, local_rows), i32),
        ),
        scratch_shapes=[
            pltpu.VMEM((local_rows, width), f32),
            pltpu.VMEM((1, local_rows), i32),
            pltpu.VMEM((1, local_rows), i32),
            pltpu.VMEM((1, cluster_count), i32),
            pltpu.SemaphoreType.DMA((4,)),
        ],
        compiler_params=params,
        name="pack",
    )(
        *[
            pltpu.with_memory_space_constraint(x, pltpu.HBM)
            for x in (
                embeddings,
                clusters.reshape(1, local_rows),
                row_ids.reshape(1, local_rows),
                owner_map.reshape(1, cluster_count),
            )
        ]
    )
    received = lax.all_to_all(packed, axes, split_axis=0, concat_axis=0, tiled=True)
    best = pl.pallas_call(
        score_kernel,
        out_shape=jax.ShapeDtypeStruct((2 * owners, lanes), f32),
        compiler_params=params,
        name="score",
    )(received)
    centroids = pl.pallas_call(
        centre_kernel,
        out_shape=jax.ShapeDtypeStruct((per_owner, width), f32),
        cost_estimate=pl.CostEstimate(
            flops=200_000_000, bytes_accessed=1_300_000, transcendentals=0
        ),
        compiler_params=params,
        name="centre",
    )(received)
    returned = lax.all_to_all(
        best.reshape(owners, 2, lanes), axes, split_axis=0, concat_axis=0, tiled=True
    )
    earlier_max = pl.pallas_call(
        unpack_kernel,
        out_shape=jax.ShapeDtypeStruct((1, local_rows), f32),
        compiler_params=params,
        name="unpack",
    )(returned.reshape(2 * owners, lanes), route)
    return (centroids, earlier_max.reshape(local_rows))


def solution(mesh):
    placed = (P(axes, None), P(axes), P(axes), P())
    return jax.shard_map(
        shards,
        mesh=mesh,
        in_specs=placed,
        out_specs=(P(axes, None), P(axes)),
        check_vma=False,
    )
```

```python
import jax
import jax.numpy as jnp
from jax import lax
from jax.experimental import pallas as pl
from jax.experimental.pallas import tpu as pltpu
from jax.sharding import PartitionSpec as P

epsilon = 1e-06
axes = ("shard", "member")
pairs = 3
slots = 2 * pairs
lanes = 128
id_base = 256
id_range = 32768
full = 32767.0
fields = 16
norm_unit = 256
norm_bytes = 6
f32 = jnp.float32
bf16 = jnp.bfloat16
i32 = jnp.int32
low_half = 0xFFFF
params = pltpu.CompilerParams(vmem_limit_bytes=24 << 20)


def iota(shape, dim):
    return lax.broadcasted_iota(i32, shape, dim)


def dot(a, b, contract=((1,), (0,))):
    return lax.dot_general(a, b, (contract, ((), ())), preferred_element_type=f32)


def one_hot(mask):
    return jnp.where(mask, 1.0, 0.0).astype(bf16)


def count(mask):
    return jnp.sum(jnp.where(mask, 1.0, 0.0), axis=0, keepdims=True)


def to_bytes(values, unit, n):
    digits = []
    rest = values * (1.0 / unit)
    for _ in range(n):
        digit = jnp.floor(rest)
        digits.append(digit)
        rest = (rest - digit) * id_base
    return digits


def pack_kernel(
    rows_hbm,
    clusters_hbm,
    ids_hbm,
    owners_hbm,
    sent_ref,
    route_ref,
    rows_ref,
    clusters_ref,
    ids_ref,
    owners_ref,
    sems,
):
    index_copies = (
        pltpu.make_async_copy(owners_hbm, owners_ref, sems.at[0]),
        pltpu.make_async_copy(clusters_hbm, clusters_ref, sems.at[1]),
        pltpu.make_async_copy(ids_hbm, ids_ref, sems.at[2]),
    )
    copy = pltpu.make_async_copy(rows_hbm, rows_ref, sems.at[3])
    for index_copy in index_copies:
        index_copy.start()
    copy.start()
    for index_copy in index_copies:
        index_copy.wait()
    clusters = clusters_ref[...]
    ids = ids_ref[...]
    owner_map = owners_ref[...].astype(f32)
    row_count, width = rows_ref.shape
    tiles = pairs * (width // lanes) + 1
    owners = sent_ref.shape[0] // tiles
    cluster_count = owner_map.shape[1]

    square = (cluster_count, cluster_count)
    diagonal = iota(square, 0) == iota(square, 1)
    before = iota(square, 0) < iota(square, 1)
    spread = jnp.where(diagonal, owner_map, 0.0).astype(bf16)
    map_col = dot(spread, jnp.ones(square, bf16))
    rank_map = count(before & (map_col == owner_map))
    sub = iota((8, cluster_count), 0)
    table = jnp.where(sub == 0, owner_map, jnp.where(sub == 1, rank_map, 0.0)).astype(bf16)
    cluster_hot = one_hot(iota((cluster_count, row_count), 0) == clusters)
    found = dot(table, cluster_hot)
    owner_col = dot(cluster_hot, map_col[:, :row_count].astype(bf16), ((0,), (0,)))
    slot = count(before & (owner_col == found[0:1])).astype(i32)
    owner = found[0:1].astype(i32)
    rank = found[1:2].astype(i32)

    copy.wait()
    rows = rows_ref[...]
    power = jnp.sum(rows * rows, axis=1, keepdims=True) + epsilon
    inverse = lax.rsqrt(power)
    norm = power * inverse
    largest = jnp.max(jnp.abs(rows), axis=1, keepdims=True) * inverse
    step = jnp.clip(jnp.ceil(largest * full), 1.0, full)
    codes = jnp.floor(rows * (inverse * (full * full / step)) + 0.5)
    upper = codes.astype(bf16)
    halves = jnp.concatenate([upper, (codes - upper.astype(f32)).astype(bf16)], axis=0)
    norm_row = jnp.sum(jnp.where(diagonal, norm, 0.0), axis=0, keepdims=True)
    step_row = jnp.sum(jnp.where(diagonal, step, 0.0), axis=0, keepdims=True)

    values = to_bytes(ids.astype(f32), id_base, 2)
    values = values + [(rank + 1).astype(f32)]
    values = values + to_bytes(step_row, id_base, 2)
    values = values + to_bytes(norm_row, norm_unit, norm_bytes)
    lane = iota((lanes, row_count), 0)
    field = jnp.where(lane // fields == slot, lane % fields, -1)
    notes = jnp.zeros((lanes, row_count), f32)
    for k, value in enumerate(values):
        notes = jnp.where(field == k, value, notes)
    notes = notes.astype(bf16)

    mine = iota((owners, row_count), 0) == owner
    takes = []
    for s in range(slots):
        take = one_hot(mine & (slot == s))
        takes.append(jnp.concatenate([take, take], axis=1))
    placed = dot(jnp.concatenate(takes, axis=0), halves).astype(i32)
    for p in range(pairs):
        even = placed[2 * p * owners : (2 * p + 1) * owners]
        odd = placed[(2 * p + 1) * owners : (2 * p + 2) * owners]
        words = (odd << 16) | (even & low_half)
        for t in range(width // lanes):
            tile = p * (width // lanes) + t
            sent_ref[pl.ds(tile, owners, tiles), :] = words[:, t * lanes : (t + 1) * lanes]
    words = dot(one_hot(mine), notes, ((1,), (1,))).astype(i32)
    sent_ref[pl.ds(tiles - 1, owners, tiles), :] = words
    sub = iota(route_ref.shape, 0)
    route_ref[...] = jnp.where(sub == 0, owner, slot)


def read_tile(got_ref, tile):
    return got_ref[pl.ds(tile, lanes, got_ref.shape[0] // lanes), :]


def read_notes(got_ref):
    return read_tile(got_ref, got_ref.shape[0] // lanes - 1).astype(f32).astype(bf16)


def read_rows(got_ref, p, steps):
    tiles = (got_ref.shape[0] // lanes - 1) // pairs
    even_step = steps[2 * p] * (1.0 / (65536.0 * full * full))
    odd_step = steps[2 * p + 1] * (1.0 / (full * full))
    even = []
    odd = []
    for t in range(tiles):
        words = read_tile(got_ref, p * tiles + t)
        even.append((words << 16).astype(f32) * even_step)
        odd.append((words >> 16).astype(f32) * odd_step)
    return [jnp.concatenate(even, axis=1), jnp.concatenate(odd, axis=1)]


def along_sublanes(notes, first, third):
    sub = iota((lanes, lanes), 0)
    field = sub % fields
    weight = jnp.where(field == first, float(id_base), 0.0)
    weight = jnp.where(field == first + 1, 1.0, weight)
    if third is not None:
        weight = jnp.where(field == third, float(id_range), weight)
    of = sub // fields
    spread = [jnp.where(of == s, weight, 0.0).astype(bf16) for s in range(slots)]
    tall = dot(notes, jnp.concatenate(spread, axis=1))
    return [tall[:, s * lanes : (s + 1) * lanes] for s in range(slots)]


def score_kernel(got_ref, best_ref):
    owners = lanes
    total = slots * owners
    notes = read_notes(got_ref)
    sub = iota((8 * slots, lanes), 0)
    field = iota((8 * slots, lanes), 1) - fields * (sub // 8)
    kind = sub % 8
    pick = jnp.where((kind == 0) & (field == 0), float(id_base), 0.0)
    pick = jnp.where((kind == 0) & (field == 1), 1.0, pick)
    pick = jnp.where((kind == 0) & (field == 2), float(id_range), pick)
    pick = jnp.where((kind == 1) & (field == 2), 1.0, pick)
    wide = dot(pick.astype(bf16), notes, ((1,), (1,)))
    high = jnp.concatenate([wide[8 * s : 8 * s + 1] for s in range(slots)], axis=1)
    low = jnp.concatenate([wide[8 * s + 1 : 8 * s + 2] for s in range(slots)], axis=1)
    low = low * float(id_range)
    key = jnp.concatenate(along_sublanes(notes, 0, 2), axis=0)
    step = along_sublanes(notes, 3, None)
    keys = []
    for p in range(pairs):
        keys = keys + [rows.astype(bf16) for rows in read_rows(got_ref, p, step)]
    keys = jnp.concatenate(keys, axis=0)

    block = 2 * lanes
    other = jnp.concatenate([key] * (block // lanes), axis=1)
    bests = []
    for start in range(0, total, block):
        stop = start + block
        scores = dot(keys, keys[start:stop], ((1,), (1,)))
        allowed = (other >= low[:, start:stop]) & (other < high[:, start:stop])
        bests.append(jnp.max(jnp.where(allowed, scores, -1.0), axis=0, keepdims=True))
    best = jnp.concatenate(bests, axis=1)
    sub = iota((lanes, owners), 0)
    rows = jnp.full((lanes, owners), -1.0, f32)
    for s in range(slots):
        rows = jnp.where(sub == s, best[:, s * owners : (s + 1) * owners], rows)
    best_ref[...] = rows.T


def centre_kernel(got_ref, sums_ref):
    owned, width = sums_ref.shape
    owners = lanes
    notes = read_notes(got_ref)
    sub = iota((8 * slots, lanes), 0)
    field = iota((8 * slots, lanes), 1) - fields * (sub // 8)
    kind = sub % 8
    pick = jnp.where((kind == 1) & (field == 2), 1.0, 0.0)
    for k in range(norm_bytes):
        weight = float(norm_unit) / float(id_base) ** k
        pick = jnp.where((kind == 0) & (field == 5 + k), weight, pick)
    wide = dot(pick.astype(bf16), notes, ((1,), (1,)))
    step = along_sublanes(notes, 3, None)

    sub = iota((8, owners), 0)
    sums = jnp.zeros((8, width), f32)
    for p in range(pairs):
        exact = jnp.concatenate(read_rows(got_ref, p, step), axis=0)
        unit = exact.astype(bf16)
        rest = (exact - unit.astype(f32)).astype(bf16)
        weights = []
        for s in (2 * p, 2 * p + 1):
            norms = wide[8 * s : 8 * s + 1]
            ranks = wide[8 * s + 1 : 8 * s + 2]
            coarse = norms.astype(bf16).astype(f32)
            weight = jnp.where(sub < owned, coarse, norms - coarse)
            weight = jnp.where(ranks == (sub % owned + 1).astype(f32), weight, 0.0)
            weights.append(jnp.where(sub < 2 * owned, weight, 0.0).astype(bf16))
        weight = jnp.concatenate(weights, axis=1)
        sums = sums + dot(weight, unit) + dot(weight, rest)
    sums = sums[0:owned] + sums[owned : 2 * owned]
    scale = lax.rsqrt(jnp.mean(sums * sums, axis=1, keepdims=True) + epsilon)
    sums_ref[...] = sums * scale


def exact_dot(values, hot, contract=((1,), (0,))):
    first = values.astype(bf16)
    rest = values - first.astype(f32)
    second = rest.astype(bf16)
    third = (rest - second.astype(f32)).astype(bf16)
    return dot(first, hot, contract) + dot(second, hot, contract) + dot(third, hot, contract)


def unpack_kernel(back_ref, route_ref, out_ref):
    owner = route_ref[0:1, :]
    slot = route_ref[1:2, :]
    back = back_ref[...]
    row_count = owner.shape[1]
    hot = one_hot(iota((back.shape[0], row_count), 0) == owner)
    found = exact_dot(back, hot, ((0,), (0,)))[0:8]
    mine = iota((8, row_count), 0) == slot
    out_ref[...] = jnp.sum(jnp.where(mine, found, 0.0), axis=0, keepdims=True)


def shards(embeddings, clusters, row_ids, owner_map):
    owners = lax.axis_size("shard") * lax.axis_size("member")
    local_rows, width = embeddings.shape
    cluster_count = owner_map.shape[0]
    per_owner = cluster_count // owners
    tiles = pairs * (width // lanes) + 1
    hbm = pl.BlockSpec(memory_space=pltpu.HBM)
    packed, route = pl.pallas_call(
        pack_kernel,
        in_specs=[hbm] * 4,
        out_shape=(
            jax.ShapeDtypeStruct((owners * tiles, lanes), i32),
            jax.ShapeDtypeStruct((8, local_rows), i32),
        ),
        scratch_shapes=[
            pltpu.VMEM((local_rows, width), f32),
            pltpu.VMEM((1, local_rows), i32),
            pltpu.VMEM((1, local_rows), i32),
            pltpu.VMEM((1, cluster_count), i32),
            pltpu.SemaphoreType.DMA((4,)),
        ],
        compiler_params=params,
        name="pack",
    )(
        *[
            pltpu.with_memory_space_constraint(x, pltpu.HBM)
            for x in (
                embeddings,
                clusters.reshape(1, local_rows),
                row_ids.reshape(1, local_rows),
                owner_map.reshape(1, cluster_count),
            )
        ]
    )
    packed = packed.reshape(owners, tiles, 1, lanes)
    received = lax.all_to_all(packed, axes, split_axis=0, concat_axis=0, tiled=True)
    received = received.reshape(owners * tiles, lanes)
    best = pl.pallas_call(
        score_kernel,
        out_shape=jax.ShapeDtypeStruct((owners, lanes), f32),
        compiler_params=params,
        name="score",
    )(received)
    centroids = pl.pallas_call(
        centre_kernel,
        out_shape=jax.ShapeDtypeStruct((per_owner, width), f32),
        cost_estimate=pl.CostEstimate(
            flops=200_000_000, bytes_accessed=1_300_000, transcendentals=0
        ),
        compiler_params=params,
        name="centre",
    )(received)
    returned = lax.all_to_all(
        best.reshape(owners, 1, lanes), axes, split_axis=0, concat_axis=0, tiled=True
    )
    earlier_max = pl.pallas_call(
        unpack_kernel,
        out_shape=jax.ShapeDtypeStruct((1, local_rows), f32),
        compiler_params=params,
        name="unpack",
    )(returned.reshape(owners, lanes), route)
    return (centroids, earlier_max.reshape(local_rows))


def solution(mesh):
    placed = (P(axes, None), P(axes), P(axes), P())
    return jax.shard_map(
        shards,
        mesh=mesh,
        in_specs=placed,
        out_specs=(P(axes, None), P(axes)),
        check_vma=False,
    )
```

```python
import jax
import jax.numpy as jnp
from jax import lax
from jax.experimental import pallas as pl
from jax.experimental.pallas import tpu as pltpu
from jax.sharding import PartitionSpec as P

epsilon = 1e-06
axes = ("shard", "member")
pairs = 3
slots = 2 * pairs
lanes = 128
id_base = 256
id_range = 32768
full = 32767.0
fields = 16
norm_unit = 256
norm_bytes = 6
f32 = jnp.float32
bf16 = jnp.bfloat16
i32 = jnp.int32
low_half = 0xFFFF
params = pltpu.CompilerParams(vmem_limit_bytes=24 << 20)


def iota(shape, dim):
    return lax.broadcasted_iota(i32, shape, dim)


def dot(a, b, contract=((1,), (0,))):
    return lax.dot_general(a, b, (contract, ((), ())), preferred_element_type=f32)


def one_hot(mask):
    return jnp.where(mask, 1.0, 0.0).astype(bf16)


def count(mask):
    return jnp.sum(jnp.where(mask, 1.0, 0.0), axis=0, keepdims=True)


def to_bytes(values, unit, n):
    digits = []
    rest = values * (1.0 / unit)
    for _ in range(n):
        digit = jnp.floor(rest)
        digits.append(digit)
        rest = (rest - digit) * id_base
    return digits


def pack_kernel(
    rows_hbm,
    clusters_hbm,
    ids_hbm,
    owners_hbm,
    sent_ref,
    route_ref,
    rows_ref,
    clusters_ref,
    ids_ref,
    owners_ref,
    sems,
):
    index_copies = (
        pltpu.make_async_copy(owners_hbm, owners_ref, sems.at[0]),
        pltpu.make_async_copy(clusters_hbm, clusters_ref, sems.at[1]),
        pltpu.make_async_copy(ids_hbm, ids_ref, sems.at[2]),
    )
    copy = pltpu.make_async_copy(rows_hbm, rows_ref, sems.at[3])
    for index_copy in index_copies:
        index_copy.start()
    copy.start()
    for index_copy in index_copies:
        index_copy.wait()
    clusters = clusters_ref[...]
    ids = ids_ref[...]
    owner_map = owners_ref[...].astype(f32)
    row_count, width = rows_ref.shape
    tiles = pairs * (width // lanes) + 1
    owners = sent_ref.shape[0] // tiles
    cluster_count = owner_map.shape[1]

    square = (cluster_count, cluster_count)
    diagonal = iota(square, 0) == iota(square, 1)
    before = iota(square, 0) < iota(square, 1)
    spread = jnp.where(diagonal, owner_map, 0.0).astype(bf16)
    map_col = dot(spread, jnp.ones(square, bf16))
    rank_map = count(before & (map_col == owner_map))
    sub = iota((8, cluster_count), 0)
    table = jnp.where(sub == 0, owner_map, jnp.where(sub == 1, rank_map, 0.0)).astype(bf16)
    cluster_hot = one_hot(iota((cluster_count, row_count), 0) == clusters)
    found = dot(table, cluster_hot)
    owner_col = dot(cluster_hot, map_col[:, :row_count].astype(bf16), ((0,), (0,)))
    slot = count(before & (owner_col == found[0:1])).astype(i32)
    owner = found[0:1].astype(i32)
    rank = found[1:2].astype(i32)

    copy.wait()
    rows = rows_ref[...]
    power = jnp.sum(rows * rows, axis=1, keepdims=True) + epsilon
    inverse = lax.rsqrt(power)
    norm = power * inverse
    largest = jnp.max(jnp.abs(rows), axis=1, keepdims=True) * inverse
    step = jnp.clip(jnp.ceil(largest * full), 1.0, full)
    codes = jnp.floor(rows * (inverse * (full * full / step)) + 0.5)
    upper = codes.astype(bf16)
    halves = jnp.concatenate([upper, (codes - upper.astype(f32)).astype(bf16)], axis=0)
    norm_row = jnp.sum(jnp.where(diagonal, norm, 0.0), axis=0, keepdims=True)
    step_row = jnp.sum(jnp.where(diagonal, step, 0.0), axis=0, keepdims=True)

    values = to_bytes(ids.astype(f32), id_base, 2)
    values = values + [(rank + 1).astype(f32)]
    values = values + to_bytes(step_row, id_base, 2)
    values = values + to_bytes(norm_row, norm_unit, norm_bytes)
    lane = iota((lanes, row_count), 0)
    field = jnp.where(lane // fields == slot, lane % fields, -1)
    notes = jnp.zeros((lanes, row_count), f32)
    for k, value in enumerate(values):
        notes = jnp.where(field == k, value, notes)
    notes = notes.astype(bf16)

    mine = iota((owners, row_count), 0) == owner
    takes = []
    for s in range(slots):
        take = one_hot(mine & (slot == s))
        takes.append(jnp.concatenate([take, take], axis=1))
    placed = dot(jnp.concatenate(takes, axis=0), halves).astype(i32)
    for p in range(pairs):
        even = placed[2 * p * owners : (2 * p + 1) * owners]
        odd = placed[(2 * p + 1) * owners : (2 * p + 2) * owners]
        words = (odd << 16) | (even & low_half)
        for t in range(width // lanes):
            tile = p * (width // lanes) + t
            sent_ref[pl.ds(tile, owners, tiles), :] = words[:, t * lanes : (t + 1) * lanes]
    words = dot(one_hot(mine), notes, ((1,), (1,))).astype(i32)
    sent_ref[pl.ds(tiles - 1, owners, tiles), :] = words
    sub = iota(route_ref.shape, 0)
    route_ref[...] = jnp.where(sub == 0, owner, slot)


def read_tile(got_ref, tile):
    return got_ref[pl.ds(tile, lanes, got_ref.shape[0] // lanes), :]


def read_notes(got_ref):
    return read_tile(got_ref, got_ref.shape[0] // lanes - 1).astype(f32).astype(bf16)


def read_rows(got_ref, p, steps):
    tiles = (got_ref.shape[0] // lanes - 1) // pairs
    even_step = steps[2 * p] * (1.0 / (65536.0 * full * full))
    odd_step = steps[2 * p + 1] * (1.0 / (full * full))
    even = []
    odd = []
    for t in range(tiles):
        words = read_tile(got_ref, p * tiles + t)
        even.append((words << 16).astype(f32) * even_step)
        odd.append((words >> 16).astype(f32) * odd_step)
    return [jnp.concatenate(even, axis=1), jnp.concatenate(odd, axis=1)]


def along_sublanes(notes, first, third):
    sub = iota((lanes, lanes), 0)
    field = sub % fields
    weight = jnp.where(field == first, float(id_base), 0.0)
    weight = jnp.where(field == first + 1, 1.0, weight)
    if third is not None:
        weight = jnp.where(field == third, float(id_range), weight)
    of = sub // fields
    spread = [jnp.where(of == s, weight, 0.0).astype(bf16) for s in range(slots)]
    tall = dot(notes, jnp.concatenate(spread, axis=1))
    return [tall[:, s * lanes : (s + 1) * lanes] for s in range(slots)]


def score_kernel(got_ref, sums_hbm, best_ref, sums_ref, sem):
    owners = lanes
    total = slots * owners
    owned, width = sums_ref.shape
    notes = read_notes(got_ref)
    sub = iota((8 * slots, lanes), 0)
    field = iota((8 * slots, lanes), 1) - fields * (sub // 8)
    kind = sub % 8
    pick = jnp.where((kind == 0) & (field == 0), float(id_base), 0.0)
    pick = jnp.where((kind == 0) & (field == 1), 1.0, pick)
    pick = jnp.where((kind == 0) & (field == 2), float(id_range), pick)
    pick = jnp.where((kind == 1) & (field == 2), 1.0, pick)
    for k in range(norm_bytes):
        weight = float(norm_unit) / float(id_base) ** k
        pick = jnp.where((kind == 2) & (field == 5 + k), weight, pick)
    wide = dot(pick.astype(bf16), notes, ((1,), (1,)))
    line = [
        jnp.concatenate([wide[8 * s + k : 8 * s + k + 1] for s in range(slots)], axis=1)
        for k in range(3)
    ]
    high = line[0]
    low = line[1] * float(id_range)
    key = jnp.concatenate(along_sublanes(notes, 0, 2), axis=0)
    step = along_sublanes(notes, 3, None)
    exact = []
    for p in range(pairs):
        exact = exact + read_rows(got_ref, p, step)
    exact = jnp.concatenate(exact, axis=0)
    keys = exact.astype(bf16)
    rest = (exact - keys.astype(f32)).astype(bf16)

    sub = iota((8, total), 0)
    coarse = line[2].astype(bf16).astype(f32)
    weight = jnp.where(sub < owned, coarse, line[2] - coarse)
    weight = jnp.where(line[1] == (sub % owned + 1).astype(f32), weight, 0.0)
    weight = jnp.where(sub < 2 * owned, weight, 0.0).astype(bf16)
    sums = dot(weight, keys) + dot(weight, rest)
    sums = sums[0:owned] + sums[owned : 2 * owned]
    scale = lax.rsqrt(jnp.mean(sums * sums, axis=1, keepdims=True) + epsilon)
    sums_ref[...] = sums * scale
    copy = pltpu.make_async_copy(sums_ref, sums_hbm, sem)
    copy.start()

    block = 2 * lanes
    other = jnp.concatenate([key] * (block // lanes), axis=1)
    bests = []
    for start in range(0, total, block):
        stop = start + block
        scores = dot(keys, keys[start:stop], ((1,), (1,)))
        allowed = (other >= low[:, start:stop]) & (other < high[:, start:stop])
        bests.append(jnp.max(jnp.where(allowed, scores, -1.0), axis=0, keepdims=True))
    best = jnp.concatenate(bests, axis=1)
    sub = iota((lanes, owners), 0)
    rows = jnp.full((lanes, owners), -1.0, f32)
    for s in range(slots):
        rows = jnp.where(sub == s, best[:, s * owners : (s + 1) * owners], rows)
    best_ref[...] = rows.T
    copy.wait()


def exact_dot(values, hot, contract=((1,), (0,))):
    first = values.astype(bf16)
    rest = values - first.astype(f32)
    second = rest.astype(bf16)
    third = (rest - second.astype(f32)).astype(bf16)
    return dot(first, hot, contract) + dot(second, hot, contract) + dot(third, hot, contract)


def unpack_kernel(back_ref, route_ref, out_ref):
    owner = route_ref[0:1, :]
    slot = route_ref[1:2, :]
    back = back_ref[...]
    row_count = owner.shape[1]
    hot = one_hot(iota((back.shape[0], row_count), 0) == owner)
    found = exact_dot(back, hot, ((0,), (0,)))[0:8]
    mine = iota((8, row_count), 0) == slot
    out_ref[...] = jnp.sum(jnp.where(mine, found, 0.0), axis=0, keepdims=True)


def shards(embeddings, clusters, row_ids, owner_map):
    owners = lax.axis_size("shard") * lax.axis_size("member")
    local_rows, width = embeddings.shape
    cluster_count = owner_map.shape[0]
    per_owner = cluster_count // owners
    tiles = pairs * (width // lanes) + 1
    hbm = pl.BlockSpec(memory_space=pltpu.HBM)
    packed, route = pl.pallas_call(
        pack_kernel,
        in_specs=[hbm] * 4,
        out_shape=(
            jax.ShapeDtypeStruct((owners * tiles, lanes), i32),
            jax.ShapeDtypeStruct((8, local_rows), i32),
        ),
        scratch_shapes=[
            pltpu.VMEM((local_rows, width), f32),
            pltpu.VMEM((1, local_rows), i32),
            pltpu.VMEM((1, local_rows), i32),
            pltpu.VMEM((1, cluster_count), i32),
            pltpu.SemaphoreType.DMA((4,)),
        ],
        compiler_params=params,
        name="pack",
    )(
        *[
            pltpu.with_memory_space_constraint(x, pltpu.HBM)
            for x in (
                embeddings,
                clusters.reshape(1, local_rows),
                row_ids.reshape(1, local_rows),
                owner_map.reshape(1, cluster_count),
            )
        ]
    )
    packed = packed.reshape(owners, tiles, 1, lanes)
    received = lax.all_to_all(packed, axes, split_axis=0, concat_axis=0, tiled=True)
    received = received.reshape(owners * tiles, lanes)
    centroids, best = pl.pallas_call(
        score_kernel,
        out_shape=(
            jax.ShapeDtypeStruct((per_owner, width), f32),
            jax.ShapeDtypeStruct((owners, lanes), f32),
        ),
        out_specs=(hbm, pl.BlockSpec(memory_space=pltpu.VMEM)),
        scratch_shapes=[pltpu.VMEM((per_owner, width), f32), pltpu.SemaphoreType.DMA(())],
        compiler_params=params,
        name="score",
    )(received)
    returned = lax.all_to_all(
        best.reshape(owners, 1, lanes), axes, split_axis=0, concat_axis=0, tiled=True
    )
    earlier_max = pl.pallas_call(
        unpack_kernel,
        out_shape=jax.ShapeDtypeStruct((1, local_rows), f32),
        compiler_params=params,
        name="unpack",
    )(returned.reshape(owners, lanes), route)
    return (centroids, earlier_max.reshape(local_rows))


def solution(mesh):
    placed = (P(axes, None), P(axes), P(axes), P())
    return jax.shard_map(
        shards,
        mesh=mesh,
        in_specs=placed,
        out_specs=(P(axes, None), P(axes)),
        check_vma=False,
    )
```

```python
import functools

import jax
import jax.numpy as jnp
from jax import lax
from jax.experimental import pallas as pl
from jax.experimental.pallas import tpu as pltpu
from jax.sharding import PartitionSpec as P

epsilon = 1e-06
axes = ("shard", "member")
exchange = ("member", "shard")
pairs = 3
slots = 2 * pairs
lanes = 128
id_base = 256
id_range = 32768
full = 32767.0
fields = 16
norm_unit = 256
norm_bytes = 6
f32 = jnp.float32
bf16 = jnp.bfloat16
i32 = jnp.int32
low_half = 0xFFFF
params = pltpu.CompilerParams(vmem_limit_bytes=24 << 20)


def iota(shape, dim):
    return lax.broadcasted_iota(i32, shape, dim)


def dot(a, b, contract=((1,), (0,))):
    return lax.dot_general(a, b, (contract, ((), ())), preferred_element_type=f32)


def one_hot(mask):
    return jnp.where(mask, 1.0, 0.0).astype(bf16)


def count(mask):
    return jnp.sum(jnp.where(mask, 1.0, 0.0), axis=0, keepdims=True)


def to_bytes(values, unit, n):
    digits = []
    rest = values * (1.0 / unit)
    for _ in range(n):
        digit = jnp.floor(rest)
        digits.append(digit)
        rest = (rest - digit) * id_base
    return digits


def pack_kernel(
    rows_hbm,
    clusters_hbm,
    ids_hbm,
    owners_hbm,
    sent_ref,
    route_ref,
    rows_ref,
    clusters_ref,
    ids_ref,
    owners_ref,
    sems,
    *,
    members,
):
    index_copies = (
        pltpu.make_async_copy(owners_hbm, owners_ref, sems.at[0]),
        pltpu.make_async_copy(clusters_hbm, clusters_ref, sems.at[1]),
        pltpu.make_async_copy(ids_hbm, ids_ref, sems.at[2]),
    )
    copy = pltpu.make_async_copy(rows_hbm, rows_ref, sems.at[3])
    for index_copy in index_copies:
        index_copy.start()
    copy.start()
    for index_copy in index_copies:
        index_copy.wait()
    clusters = clusters_ref[...]
    ids = ids_ref[...]
    owner_map = owners_ref[...]
    owner_map = owner_map % members * (lanes // members) + owner_map // members
    owner_map = owner_map.astype(f32)
    row_count, width = rows_ref.shape
    tiles = pairs * (width // lanes) + 1
    owners = sent_ref.shape[0] // tiles
    cluster_count = owner_map.shape[1]

    square = (cluster_count, cluster_count)
    diagonal = iota(square, 0) == iota(square, 1)
    before = iota(square, 0) < iota(square, 1)
    spread = jnp.where(diagonal, owner_map, 0.0).astype(bf16)
    map_col = dot(spread, jnp.ones(square, bf16))
    rank_map = count(before & (map_col == owner_map))
    sub = iota((8, cluster_count), 0)
    table = jnp.where(sub == 0, owner_map, jnp.where(sub == 1, rank_map, 0.0)).astype(bf16)
    cluster_hot = one_hot(iota((cluster_count, row_count), 0) == clusters)
    found = dot(table, cluster_hot)
    owner_col = dot(cluster_hot, map_col[:, :row_count].astype(bf16), ((0,), (0,)))
    slot = count(before & (owner_col == found[0:1])).astype(i32)
    owner = found[0:1].astype(i32)
    rank = found[1:2].astype(i32)

    copy.wait()
    rows = rows_ref[...]
    power = jnp.sum(rows * rows, axis=1, keepdims=True) + epsilon
    inverse = lax.rsqrt(power)
    norm = power * inverse
    largest = jnp.max(jnp.abs(rows), axis=1, keepdims=True) * inverse
    step = jnp.clip(jnp.ceil(largest * full), 1.0, full)
    codes = jnp.floor(rows * (inverse * (full * full / step)) + 0.5)
    upper = codes.astype(bf16)
    halves = jnp.concatenate([upper, (codes - upper.astype(f32)).astype(bf16)], axis=0)
    norm_row = jnp.sum(jnp.where(diagonal, norm, 0.0), axis=0, keepdims=True)
    step_row = jnp.sum(jnp.where(diagonal, step, 0.0), axis=0, keepdims=True)

    side = (2 * rank - 1).astype(f32)
    values = [side * digit for digit in to_bytes((id_range - ids).astype(f32), id_base, 2)]
    values = values + [(rank + 1).astype(f32)]
    values = values + to_bytes(step_row, id_base, 2)
    values = values + to_bytes(norm_row, norm_unit, norm_bytes)
    lane = iota((lanes, row_count), 0)
    field = jnp.where(lane // fields == slot, lane % fields, -1)
    notes = jnp.zeros((lanes, row_count), f32)
    for k, value in enumerate(values):
        notes = jnp.where(field == k, value, notes)
    notes = notes.astype(bf16)

    mine = iota((owners, row_count), 0) == owner
    takes = []
    for s in range(slots):
        take = one_hot(mine & (slot == s))
        takes.append(jnp.concatenate([take, take], axis=1))
    placed = dot(jnp.concatenate(takes, axis=0), halves).astype(i32)
    for p in range(pairs):
        even = placed[2 * p * owners : (2 * p + 1) * owners]
        odd = placed[(2 * p + 1) * owners : (2 * p + 2) * owners]
        words = (odd << 16) | (even & low_half)
        for t in range(width // lanes):
            tile = p * (width // lanes) + t
            sent_ref[pl.ds(tile, owners, tiles), :] = words[:, t * lanes : (t + 1) * lanes]
    words = dot(one_hot(mine), notes, ((1,), (1,))).astype(i32)
    sent_ref[pl.ds(tiles - 1, owners, tiles), :] = words
    sub = iota(route_ref.shape, 0)
    route_ref[...] = jnp.where(sub == 0, owner, slot)


def read_tile(got_ref, tile):
    return got_ref[pl.ds(tile, lanes, got_ref.shape[0] // lanes), :]


def read_notes(got_ref):
    return read_tile(got_ref, got_ref.shape[0] // lanes - 1).astype(f32).astype(bf16)


def read_rows(got_ref, p, steps):
    tiles = (got_ref.shape[0] // lanes - 1) // pairs
    even_step = steps[2 * p] * (1.0 / (65536.0 * full * full))
    odd_step = steps[2 * p + 1] * (1.0 / (full * full))
    even = []
    odd = []
    for t in range(tiles):
        words = read_tile(got_ref, p * tiles + t)
        even.append((words << 16).astype(f32) * even_step)
        odd.append((words >> 16).astype(f32) * odd_step)
    return [jnp.concatenate(even, axis=1), jnp.concatenate(odd, axis=1)]


def along_sublanes(notes, first):
    sub = iota((lanes, lanes), 0)
    field = sub % fields
    weight = jnp.where(field == first, float(id_base), 0.0)
    weight = jnp.where(field == first + 1, 1.0, weight)
    of = sub // fields
    spread = [jnp.where(of == s, weight, 0.0).astype(bf16) for s in range(slots)]
    tall = dot(notes, jnp.concatenate(spread, axis=1))
    return [tall[:, s * lanes : (s + 1) * lanes] for s in range(slots)]


def score_kernel(got_ref, sums_hbm, best_ref, sums_ref, sem):
    owners = lanes
    total = slots * owners
    owned, width = sums_ref.shape
    notes = read_notes(got_ref)
    sub = iota((8 * slots, lanes), 0)
    field = iota((8 * slots, lanes), 1) - fields * (sub // 8)
    kind = sub % 8
    pick = jnp.where((kind == 0) & (field == 0), float(id_base), 0.0)
    pick = jnp.where((kind == 0) & (field == 1), 1.0, pick)
    pick = jnp.where((kind == 1) & (field == 2), 1.0, pick)
    for k in range(norm_bytes):
        weight = float(norm_unit) / float(id_base) ** k
        pick = jnp.where((kind == 2) & (field == 5 + k), weight, pick)
    wide = dot(pick.astype(bf16), notes, ((1,), (1,)))
    line = [
        jnp.concatenate([wide[8 * s + k : 8 * s + k + 1] for s in range(slots)], axis=1)
        for k in range(3)
    ]
    side = jnp.where(line[0] > 0.0, 1.0, -1.0)
    size = jnp.abs(line[0])
    key = jnp.concatenate(along_sublanes(notes, 0), axis=0)
    step = along_sublanes(notes, 3)
    exact = []
    for p in range(pairs):
        exact = exact + read_rows(got_ref, p, step)
    exact = jnp.concatenate(exact, axis=0)
    keys = exact.astype(bf16)
    rest = (exact - keys.astype(f32)).astype(bf16)

    copy = pltpu.make_async_copy(sums_ref, sums_hbm, sem)

    def centre():
        sub = iota((8, total), 0)
        coarse = line[2].astype(bf16).astype(f32)
        weight = jnp.where(sub < owned, coarse, line[2] - coarse)
        weight = jnp.where(line[1] == (sub % owned + 1).astype(f32), weight, 0.0)
        weight = jnp.where(sub < 2 * owned, weight, 0.0).astype(bf16)
        sums = dot(weight, keys) + dot(weight, rest)
        sums = sums[0:owned] + sums[owned : 2 * owned]
        scale = lax.rsqrt(jnp.mean(sums * sums, axis=1, keepdims=True) + epsilon)
        sums_ref[...] = sums * scale
        copy.start()

    block = 2 * lanes
    other = jnp.concatenate([key] * (block // lanes), axis=1)
    bests = []
    for start in range(0, total, block):
        if start == 1 * block:
            centre()
        stop = start + block
        scores = dot(keys, keys[start:stop], ((1,), (1,)))
        allowed = other * side[:, start:stop] > size[:, start:stop]
        bests.append(jnp.max(jnp.where(allowed, scores, -1.0), axis=0, keepdims=True))
    best = jnp.concatenate(bests, axis=1)
    sub = iota((lanes, owners), 0)
    rows = jnp.full((lanes, owners), -1.0, f32)
    for s in range(slots):
        rows = jnp.where(sub == s, best[:, s * owners : (s + 1) * owners], rows)
    best_ref[...] = rows.T
    copy.wait()


def exact_dot(values, hot, contract=((1,), (0,))):
    first = values.astype(bf16)
    rest = values - first.astype(f32)
    second = rest.astype(bf16)
    third = (rest - second.astype(f32)).astype(bf16)
    return dot(first, hot, contract) + dot(second, hot, contract) + dot(third, hot, contract)


def unpack_kernel(back_ref, route_ref, out_ref):
    owner = route_ref[0:1, :]
    slot = route_ref[1:2, :]
    back = back_ref[...]
    row_count = owner.shape[1]
    hot = one_hot(iota((back.shape[0], row_count), 0) == owner)
    found = exact_dot(back, hot, ((0,), (0,)))[0:8]
    mine = iota((8, row_count), 0) == slot
    out_ref[...] = jnp.sum(jnp.where(mine, found, 0.0), axis=0, keepdims=True)


def shards(embeddings, clusters, row_ids, owner_map):
    owners = lax.axis_size("shard") * lax.axis_size("member")
    local_rows, width = embeddings.shape
    cluster_count = owner_map.shape[0]
    per_owner = cluster_count // owners
    tiles = pairs * (width // lanes) + 1
    hbm = pl.BlockSpec(memory_space=pltpu.HBM)
    packed, route = pl.pallas_call(
        functools.partial(pack_kernel, members=lax.axis_size("member")),
        in_specs=[hbm] * 4,
        out_shape=(
            jax.ShapeDtypeStruct((owners * tiles, lanes), i32),
            jax.ShapeDtypeStruct((8, local_rows), i32),
        ),
        scratch_shapes=[
            pltpu.VMEM((local_rows, width), f32),
            pltpu.VMEM((1, local_rows), i32),
            pltpu.VMEM((1, local_rows), i32),
            pltpu.VMEM((1, cluster_count), i32),
            pltpu.SemaphoreType.DMA((4,)),
        ],
        compiler_params=params,
        name="pack",
    )(
        *[
            pltpu.with_memory_space_constraint(x, pltpu.HBM)
            for x in (
                embeddings,
                clusters.reshape(1, local_rows),
                row_ids.reshape(1, local_rows),
                owner_map.reshape(1, cluster_count),
            )
        ]
    )
    packed = packed.reshape(owners, tiles, 1, lanes)
    received = lax.all_to_all(packed, exchange, split_axis=0, concat_axis=0, tiled=True)
    received = received.reshape(owners * tiles, lanes)
    centroids, best = pl.pallas_call(
        score_kernel,
        out_shape=(
            jax.ShapeDtypeStruct((per_owner, width), f32),
            jax.ShapeDtypeStruct((owners, lanes), f32),
        ),
        out_specs=(hbm, pl.BlockSpec(memory_space=pltpu.VMEM)),
        scratch_shapes=[pltpu.VMEM((per_owner, width), f32), pltpu.SemaphoreType.DMA(())],
        compiler_params=params,
        name="score",
    )(received)
    returned = lax.all_to_all(
        best.reshape(owners, 1, lanes), exchange, split_axis=0, concat_axis=0, tiled=True
    )
    earlier_max = pl.pallas_call(
        unpack_kernel,
        out_shape=jax.ShapeDtypeStruct((1, local_rows), f32),
        compiler_params=params,
        name="unpack",
    )(returned.reshape(owners, lanes), route)
    return (centroids, earlier_max.reshape(local_rows))


def solution(mesh):
    placed = (P(axes, None), P(axes), P(axes), P())
    return jax.shard_map(
        shards,
        mesh=mesh,
        in_specs=placed,
        out_specs=(P(axes, None), P(axes)),
        check_vma=False,
    )
```

```python
import functools

import jax
import jax.numpy as jnp
from jax import lax
from jax.experimental import pallas as pl
from jax.experimental.pallas import tpu as pltpu
from jax.sharding import PartitionSpec as P

epsilon = 1e-06
axes = ("shard", "member")
pairs = 3
slots = 2 * pairs
lanes = 128
half = 64
id_base = 256
id_range = 32768
full = 32767.0
fields = 16
norm_unit = 256
norm_bytes = 6
f32 = jnp.float32
bf16 = jnp.bfloat16
i32 = jnp.int32
low_half = 0xFFFF
params = pltpu.CompilerParams(vmem_limit_bytes=24 << 20)


def iota(shape, dim):
    return lax.broadcasted_iota(i32, shape, dim)


def dot(a, b, contract=((1,), (0,))):
    return lax.dot_general(a, b, (contract, ((), ())), preferred_element_type=f32)


def one_hot(mask):
    return jnp.where(mask, 1.0, 0.0).astype(bf16)


def count(mask):
    return jnp.sum(jnp.where(mask, 1.0, 0.0), axis=0, keepdims=True)


def to_bytes(values, unit, n):
    digits = []
    rest = values * (1.0 / unit)
    for _ in range(n):
        digit = jnp.floor(rest)
        digits.append(digit)
        rest = (rest - digit) * id_base
    return digits


def pack_kernel(
    rows_hbm,
    clusters_hbm,
    ids_hbm,
    owners_hbm,
    sent_ref,
    route_ref,
    rows_ref,
    clusters_ref,
    ids_ref,
    owners_ref,
    sems,
    *,
    members,
):
    index_copies = (
        pltpu.make_async_copy(owners_hbm, owners_ref, sems.at[0]),
        pltpu.make_async_copy(clusters_hbm, clusters_ref, sems.at[1]),
        pltpu.make_async_copy(ids_hbm, ids_ref, sems.at[2]),
    )
    copy = pltpu.make_async_copy(rows_hbm, rows_ref, sems.at[3])
    for index_copy in index_copies:
        index_copy.start()
    copy.start()
    for index_copy in index_copies:
        index_copy.wait()
    clusters = clusters_ref[...]
    ids = ids_ref[...]
    owner_map = owners_ref[...].astype(f32)
    row_count, width = rows_ref.shape
    tiles = pairs * (width // lanes) + 1
    owners = sent_ref.shape[0] // tiles
    cluster_count = owner_map.shape[1]

    square = (cluster_count, cluster_count)
    diagonal = iota(square, 0) == iota(square, 1)
    before = iota(square, 0) < iota(square, 1)
    spread = jnp.where(diagonal, owner_map, 0.0).astype(bf16)
    map_col = dot(spread, jnp.ones(square, bf16))
    rank_map = count(before & (map_col == owner_map))
    sub = iota((8, cluster_count), 0)
    table = jnp.where(sub == 0, owner_map, jnp.where(sub == 1, rank_map, 0.0)).astype(bf16)
    cluster_hot = one_hot(iota((cluster_count, row_count), 0) == clusters)
    found = dot(table, cluster_hot)
    owner_col = dot(cluster_hot, map_col[:, :row_count].astype(bf16), ((0,), (0,)))
    slot = count(before & (owner_col == found[0:1])).astype(i32)
    owner = found[0:1].astype(i32)
    rank = found[1:2].astype(i32)

    copy.wait()
    rows = rows_ref[...]
    power = jnp.sum(rows * rows, axis=1, keepdims=True) + epsilon
    inverse = lax.rsqrt(power)
    norm = power * inverse
    largest = jnp.max(jnp.abs(rows), axis=1, keepdims=True) * inverse
    step = jnp.clip(jnp.ceil(largest * full), 1.0, full)
    codes = jnp.floor(rows * (inverse * (full * full / step)) + 0.5)
    upper = codes.astype(bf16)
    halves = jnp.concatenate([upper, (codes - upper.astype(f32)).astype(bf16)], axis=0)
    norm_row = jnp.sum(jnp.where(diagonal, norm, 0.0), axis=0, keepdims=True)
    step_row = jnp.sum(jnp.where(diagonal, step, 0.0), axis=0, keepdims=True)

    side = (2 * rank - 1).astype(f32)
    values = [side * digit for digit in to_bytes((id_range - ids).astype(f32), id_base, 2)]
    values = values + [(rank + 1).astype(f32)]
    values = values + to_bytes(step_row, id_base, 2)
    values = values + to_bytes(norm_row, norm_unit, norm_bytes)
    lane = iota((lanes, row_count), 0)
    field = jnp.where(lane // fields == slot, lane % fields, -1)
    notes = jnp.zeros((lanes, row_count), f32)
    for k, value in enumerate(values):
        notes = jnp.where(field == k, value, notes)
    notes = notes.astype(bf16)

    chip = owner // (2 * members) * members + owner % members
    other = owner // members % 2 != lax.axis_index("shard") % 2
    mine = iota((owners, row_count), 0) == 2 * chip + jnp.where(other, 1, 0)
    takes = []
    for s in range(slots):
        take = one_hot(mine & (slot == s))
        takes.append(jnp.concatenate([take, take], axis=1))
    placed = dot(jnp.concatenate(takes, axis=0), halves).astype(i32)
    for p in range(pairs):
        even = placed[2 * p * owners : (2 * p + 1) * owners]
        odd = placed[(2 * p + 1) * owners : (2 * p + 2) * owners]
        words = (odd << 16) | (even & low_half)
        for t in range(width // lanes):
            tile = p * (width // lanes) + t
            sent_ref[pl.ds(tile, owners, tiles), :] = words[:, t * lanes : (t + 1) * lanes]
    words = dot(one_hot(mine), notes, ((1,), (1,))).astype(i32)
    sent_ref[pl.ds(tiles - 1, owners, tiles), :] = words
    sub = iota(route_ref.shape, 0)
    route_ref[...] = jnp.where(sub == 0, owner, slot)


def split_kernel(got_ref, other_ref):
    tiles = other_ref.shape[0] // half
    for t in range(tiles):
        words = got_ref[pl.ds(tiles + t, half, 2 * tiles), :]
        other_ref[pl.ds(t, half, tiles), :] = words


def read_tile(got_refs, tile):
    mine_ref, other_ref = got_refs
    tiles = other_ref.shape[0] // half
    mine = mine_ref[pl.ds(tile, half, 2 * tiles), :]
    return jnp.concatenate([mine, other_ref[pl.ds(tile, half, tiles), :]], axis=0)


def read_notes(got_refs):
    return read_tile(got_refs, got_refs[1].shape[0] // half - 1).astype(f32).astype(bf16)


def read_rows(got_refs, p, steps):
    tiles = (got_refs[1].shape[0] // half - 1) // pairs
    even_step = steps[2 * p] * (1.0 / (65536.0 * full * full))
    odd_step = steps[2 * p + 1] * (1.0 / (full * full))
    even = []
    odd = []
    for t in range(tiles):
        words = read_tile(got_refs, p * tiles + t)
        even.append((words << 16).astype(f32) * even_step)
        odd.append((words >> 16).astype(f32) * odd_step)
    return [jnp.concatenate(even, axis=1), jnp.concatenate(odd, axis=1)]


def along_sublanes(notes, first):
    sub = iota((lanes, lanes), 0)
    field = sub % fields
    weight = jnp.where(field == first, float(id_base), 0.0)
    weight = jnp.where(field == first + 1, 1.0, weight)
    of = sub // fields
    spread = [jnp.where(of == s, weight, 0.0).astype(bf16) for s in range(slots)]
    tall = dot(notes, jnp.concatenate(spread, axis=1))
    return [tall[:, s * lanes : (s + 1) * lanes] for s in range(slots)]


def score_kernel(mine_ref, other_ref, sums_hbm, best_ref, sums_ref, sem, *, members):
    got_refs = (mine_ref, other_ref)
    owners = lanes
    total = slots * owners
    owned, width = sums_ref.shape
    notes = read_notes(got_refs)
    sub = iota((8 * slots, lanes), 0)
    field = iota((8 * slots, lanes), 1) - fields * (sub // 8)
    kind = sub % 8
    pick = jnp.where((kind == 0) & (field == 0), float(id_base), 0.0)
    pick = jnp.where((kind == 0) & (field == 1), 1.0, pick)
    pick = jnp.where((kind == 1) & (field == 2), 1.0, pick)
    for k in range(norm_bytes):
        weight = float(norm_unit) / float(id_base) ** k
        pick = jnp.where((kind == 2) & (field == 5 + k), weight, pick)
    wide = dot(pick.astype(bf16), notes, ((1,), (1,)))
    line = [
        jnp.concatenate([wide[8 * s + k : 8 * s + k + 1] for s in range(slots)], axis=1)
        for k in range(3)
    ]
    side = jnp.where(line[0] > 0.0, 1.0, -1.0)
    size = jnp.abs(line[0])
    key = jnp.concatenate(along_sublanes(notes, 0), axis=0)
    step = along_sublanes(notes, 3)
    exact = []
    for p in range(pairs):
        exact = exact + read_rows(got_refs, p, step)
    exact = jnp.concatenate(exact, axis=0)
    keys = exact.astype(bf16)
    rest = (exact - keys.astype(f32)).astype(bf16)

    copy = pltpu.make_async_copy(sums_ref, sums_hbm, sem)

    def centre():
        sub = iota((8, total), 0)
        coarse = line[2].astype(bf16).astype(f32)
        weight = jnp.where(sub < owned, coarse, line[2] - coarse)
        weight = jnp.where(line[1] == (sub % owned + 1).astype(f32), weight, 0.0)
        weight = jnp.where(sub < 2 * owned, weight, 0.0).astype(bf16)
        sums = dot(weight, keys) + dot(weight, rest)
        sums = sums[0:owned] + sums[owned : 2 * owned]
        scale = lax.rsqrt(jnp.mean(sums * sums, axis=1, keepdims=True) + epsilon)
        sums_ref[...] = sums * scale
        copy.start()

    block = 2 * lanes
    other = jnp.concatenate([key] * (block // lanes), axis=1)
    bests = []
    for start in range(0, total, block):
        if start == 0 * block:
            centre()
        stop = start + block
        scores = dot(keys, keys[start:stop], ((1,), (1,)))
        allowed = other * side[:, start:stop] > size[:, start:stop]
        bests.append(jnp.max(jnp.where(allowed, scores, -1.0), axis=0, keepdims=True))
    best = jnp.concatenate(bests, axis=1)
    sub = iota((lanes, owners), 0)
    rows = jnp.full((lanes, owners), -1.0, f32)
    for s in range(slots):
        rows = jnp.where(sub == s, best[:, s * owners : (s + 1) * owners], rows)
    rows = rows.T
    north = jnp.broadcast_to(lax.axis_index("shard") % 2, (members, lanes)) == 1
    for x in range(half // members):
        first = rows[x * members : (x + 1) * members]
        second = rows[half + x * members : half + (x + 1) * members]
        at = 2 * x * members
        best_ref[at : at + members, :] = jnp.where(north, second, first)
        best_ref[at + members : at + 2 * members, :] = jnp.where(north, first, second)
    copy.wait()


def exact_dot(values, hot, contract=((1,), (0,))):
    first = values.astype(bf16)
    rest = values - first.astype(f32)
    second = rest.astype(bf16)
    third = (rest - second.astype(f32)).astype(bf16)
    return dot(first, hot, contract) + dot(second, hot, contract) + dot(third, hot, contract)


def unpack_kernel(back_ref, route_ref, out_ref):
    owner = route_ref[0:1, :]
    slot = route_ref[1:2, :]
    back = back_ref[...]
    row_count = owner.shape[1]
    hot = one_hot(iota((back.shape[0], row_count), 0) == owner)
    found = exact_dot(back, hot, ((0,), (0,)))[0:8]
    mine = iota((8, row_count), 0) == slot
    out_ref[...] = jnp.sum(jnp.where(mine, found, 0.0), axis=0, keepdims=True)


def shards(embeddings, clusters, row_ids, owner_map):
    shard_count = lax.axis_size("shard")
    members = lax.axis_size("member")
    owners = shard_count * members
    local_rows, width = embeddings.shape
    cluster_count = owner_map.shape[0]
    per_owner = cluster_count // owners
    tiles = pairs * (width // lanes) + 1
    hbm = pl.BlockSpec(memory_space=pltpu.HBM)
    packed, route = pl.pallas_call(
        functools.partial(pack_kernel, members=members),
        in_specs=[hbm] * 4,
        out_shape=(
            jax.ShapeDtypeStruct((owners * tiles, lanes), i32),
            jax.ShapeDtypeStruct((8, local_rows), i32),
        ),
        scratch_shapes=[
            pltpu.VMEM((local_rows, width), f32),
            pltpu.VMEM((1, local_rows), i32),
            pltpu.VMEM((1, local_rows), i32),
            pltpu.VMEM((1, cluster_count), i32),
            pltpu.SemaphoreType.DMA((4,)),
        ],
        compiler_params=params,
        name="pack",
    )(
        *[
            pltpu.with_memory_space_constraint(x, pltpu.HBM)
            for x in (
                embeddings,
                clusters.reshape(1, local_rows),
                row_ids.reshape(1, local_rows),
                owner_map.reshape(1, cluster_count),
            )
        ]
    )
    packed = packed.reshape(half, 2 * tiles, 1, lanes)
    groups = [
        [s * members + m for s in range(parity, shard_count, 2) for m in range(members)]
        for parity in range(2)
    ]
    received = lax.all_to_all(
        packed, axes, split_axis=0, concat_axis=0, tiled=True, axis_index_groups=groups
    )
    received = received.reshape(owners * tiles, lanes)
    other = pl.pallas_call(
        split_kernel,
        out_shape=jax.ShapeDtypeStruct((half * tiles, lanes), i32),
        compiler_params=params,
        name="split",
    )(received)
    other = lax.ppermute(other, "shard", [(s, s ^ 1) for s in range(shard_count)])
    centroids, best = pl.pallas_call(
        functools.partial(score_kernel, members=members),
        out_shape=(
            jax.ShapeDtypeStruct((per_owner, width), f32),
            jax.ShapeDtypeStruct((owners, lanes), f32),
        ),
        out_specs=(hbm, pl.BlockSpec(memory_space=pltpu.VMEM)),
        scratch_shapes=[pltpu.VMEM((per_owner, width), f32), pltpu.SemaphoreType.DMA(())],
        compiler_params=params,
        name="score",
    )(received, other)
    returned = lax.all_to_all(
        best.reshape(owners, 1, lanes), axes, split_axis=0, concat_axis=0, tiled=True
    )
    earlier_max = pl.pallas_call(
        unpack_kernel,
        out_shape=jax.ShapeDtypeStruct((1, local_rows), f32),
        compiler_params=params,
        name="unpack",
    )(returned.reshape(owners, lanes), route)
    return (centroids, earlier_max.reshape(local_rows))


def solution(mesh):
    placed = (P(axes, None), P(axes), P(axes), P())
    return jax.shard_map(
        shards,
        mesh=mesh,
        in_specs=placed,
        out_specs=(P(axes, None), P(axes)),
        check_vma=False,
    )
```

```python
import functools

import jax
import jax.numpy as jnp
from jax import lax
from jax.experimental import pallas as pl
from jax.experimental.pallas import tpu as pltpu
from jax.sharding import PartitionSpec as P

epsilon = 1e-06
axes = ("shard", "member")
exchange = ("member", "shard")
pairs = 3
slots = 2 * pairs
lanes = 128
id_base = 256
id_range = 32768
full = 32767.0
fields = 16
norm_unit = 256
norm_bytes = 6
f32 = jnp.float32
bf16 = jnp.bfloat16
i32 = jnp.int32
low_half = 0xFFFF
params = pltpu.CompilerParams(vmem_limit_bytes=24 << 20)


def iota(shape, dim):
    return lax.broadcasted_iota(i32, shape, dim)


def dot(a, b, contract=((1,), (0,))):
    return lax.dot_general(a, b, (contract, ((), ())), preferred_element_type=f32)


def one_hot(mask):
    return jnp.where(mask, 1.0, 0.0).astype(bf16)


def count(mask):
    return jnp.sum(jnp.where(mask, 1.0, 0.0), axis=0, keepdims=True)


def to_bytes(values, unit, n):
    digits = []
    rest = values * (1.0 / unit)
    for _ in range(n):
        digit = jnp.floor(rest)
        digits.append(digit)
        rest = (rest - digit) * id_base
    return digits


def pack_kernel(
    rows_hbm,
    clusters_hbm,
    ids_hbm,
    owners_hbm,
    sent_ref,
    route_ref,
    rows_ref,
    clusters_ref,
    ids_ref,
    owners_ref,
    sems,
    *,
    members,
):
    index_copies = (
        pltpu.make_async_copy(owners_hbm, owners_ref, sems.at[0]),
        pltpu.make_async_copy(clusters_hbm, clusters_ref, sems.at[1]),
        pltpu.make_async_copy(ids_hbm, ids_ref, sems.at[2]),
    )
    copy = pltpu.make_async_copy(rows_hbm, rows_ref, sems.at[3])
    for index_copy in index_copies:
        index_copy.start()
    copy.start()
    for index_copy in index_copies:
        index_copy.wait()
    clusters = clusters_ref[...]
    ids = ids_ref[...]
    owner_map = owners_ref[...]
    owner_map = owner_map % members * (lanes // members) + owner_map // members
    owner_map = owner_map.astype(f32)
    row_count, width = rows_ref.shape
    tiles = pairs * (width // lanes) + 1
    owners = sent_ref.shape[0] // tiles
    cluster_count = owner_map.shape[1]

    square = (cluster_count, cluster_count)
    diagonal = iota(square, 0) == iota(square, 1)
    before = iota(square, 0) < iota(square, 1)
    spread = jnp.where(diagonal, owner_map, 0.0).astype(bf16)
    map_col = dot(spread, jnp.ones(square, bf16))
    rank_map = count(before & (map_col == owner_map))
    sub = iota((8, cluster_count), 0)
    table = jnp.where(sub == 0, owner_map, jnp.where(sub == 1, rank_map, 0.0)).astype(bf16)
    cluster_hot = one_hot(iota((cluster_count, row_count), 0) == clusters)
    found = dot(table, cluster_hot)
    owner_col = dot(cluster_hot, map_col[:, :row_count].astype(bf16), ((0,), (0,)))
    slot = count(before & (owner_col == found[0:1])).astype(i32)
    owner = found[0:1].astype(i32)
    rank = found[1:2].astype(i32)

    copy.wait()
    rows = rows_ref[...]
    power = jnp.sum(rows * rows, axis=1, keepdims=True) + epsilon
    inverse = lax.rsqrt(power)
    norm = power * inverse
    largest = jnp.max(jnp.abs(rows), axis=1, keepdims=True) * inverse
    step = jnp.clip(jnp.ceil(largest * full), 1.0, full)
    codes = jnp.floor(rows * (inverse * (full * full / step)) + 0.5)
    upper = codes.astype(bf16)
    halves = jnp.concatenate([upper, (codes - upper.astype(f32)).astype(bf16)], axis=0)
    norm_row = jnp.sum(jnp.where(diagonal, norm, 0.0), axis=0, keepdims=True)
    step_row = jnp.sum(jnp.where(diagonal, step, 0.0), axis=0, keepdims=True)

    side = (2 * rank - 1).astype(f32)
    values = [side * digit for digit in to_bytes((id_range - ids).astype(f32), id_base, 2)]
    values = values + [(rank + 1).astype(f32)]
    values = values + to_bytes(step_row, id_base, 2)
    values = values + to_bytes(norm_row, norm_unit, norm_bytes)
    lane = iota((lanes, row_count), 0)
    field = jnp.where(lane // fields == slot, lane % fields, -1)
    notes = jnp.zeros((lanes, row_count), f32)
    for k, value in enumerate(values):
        notes = jnp.where(field == k, value, notes)
    notes = notes.astype(bf16)

    mine = iota((owners, row_count), 0) == owner
    takes = []
    for s in range(slots):
        take = one_hot(mine & (slot == s))
        takes.append(jnp.concatenate([take, take], axis=1))
    placed = dot(jnp.concatenate(takes, axis=0), halves).astype(i32)
    for p in range(pairs):
        even = placed[2 * p * owners : (2 * p + 1) * owners]
        odd = placed[(2 * p + 1) * owners : (2 * p + 2) * owners]
        words = (odd << 16) | (even & low_half)
        for t in range(width // lanes):
            tile = p * (width // lanes) + t
            sent_ref[pl.ds(tile, owners, tiles), :] = words[:, t * lanes : (t + 1) * lanes]
    words = dot(one_hot(mine), notes, ((1,), (1,))).astype(i32)
    sent_ref[pl.ds(tiles - 1, owners, tiles), :] = words
    sub = iota(route_ref.shape, 0)
    shard_count = owners // members
    owner = owner % shard_count * members + owner // shard_count
    route_ref[...] = jnp.where(sub == 0, owner, slot)


def read_tile(got_ref, tile):
    return got_ref[pl.ds(tile, lanes, got_ref.shape[0] // lanes), :]


def read_notes(got_ref):
    return read_tile(got_ref, got_ref.shape[0] // lanes - 1).astype(f32).astype(bf16)


def read_rows(got_ref, p, steps):
    tiles = (got_ref.shape[0] // lanes - 1) // pairs
    even_step = steps[2 * p] * (1.0 / (65536.0 * full * full))
    odd_step = steps[2 * p + 1] * (1.0 / (full * full))
    even = []
    odd = []
    for t in range(tiles):
        words = read_tile(got_ref, p * tiles + t)
        even.append((words << 16).astype(f32) * even_step)
        odd.append((words >> 16).astype(f32) * odd_step)
    return [jnp.concatenate(even, axis=1), jnp.concatenate(odd, axis=1)]


def along_sublanes(notes, first):
    sub = iota((lanes, lanes), 0)
    field = sub % fields
    weight = jnp.where(field == first, float(id_base), 0.0)
    weight = jnp.where(field == first + 1, 1.0, weight)
    of = sub // fields
    spread = [jnp.where(of == s, weight, 0.0).astype(bf16) for s in range(slots)]
    tall = dot(notes, jnp.concatenate(spread, axis=1))
    return [tall[:, s * lanes : (s + 1) * lanes] for s in range(slots)]


def score_kernel(got_ref, sums_hbm, best_ref, sums_ref, sem, *, members):
    owners = lanes
    total = slots * owners
    owned, width = sums_ref.shape
    notes = read_notes(got_ref)
    sub = iota((8 * slots, lanes), 0)
    field = iota((8 * slots, lanes), 1) - fields * (sub // 8)
    kind = sub % 8
    pick = jnp.where((kind == 0) & (field == 0), float(id_base), 0.0)
    pick = jnp.where((kind == 0) & (field == 1), 1.0, pick)
    pick = jnp.where((kind == 1) & (field == 2), 1.0, pick)
    for k in range(norm_bytes):
        weight = float(norm_unit) / float(id_base) ** k
        pick = jnp.where((kind == 2) & (field == 5 + k), weight, pick)
    wide = dot(pick.astype(bf16), notes, ((1,), (1,)))
    line = [
        jnp.concatenate([wide[8 * s + k : 8 * s + k + 1] for s in range(slots)], axis=1)
        for k in range(3)
    ]
    side = jnp.where(line[0] > 0.0, 1.0, -1.0)
    size = jnp.abs(line[0])
    key = jnp.concatenate(along_sublanes(notes, 0), axis=0)
    step = along_sublanes(notes, 3)
    exact = []
    for p in range(pairs):
        exact = exact + read_rows(got_ref, p, step)
    exact = jnp.concatenate(exact, axis=0)
    keys = exact.astype(bf16)
    rest = (exact - keys.astype(f32)).astype(bf16)

    copy = pltpu.make_async_copy(sums_ref, sums_hbm, sem)

    def centre():
        sub = iota((8, total), 0)
        coarse = line[2].astype(bf16).astype(f32)
        weight = jnp.where(sub < owned, coarse, line[2] - coarse)
        weight = jnp.where(line[1] == (sub % owned + 1).astype(f32), weight, 0.0)
        weight = jnp.where(sub < 2 * owned, weight, 0.0).astype(bf16)
        sums = dot(weight, keys) + dot(weight, rest)
        sums = sums[0:owned] + sums[owned : 2 * owned]
        scale = lax.rsqrt(jnp.mean(sums * sums, axis=1, keepdims=True) + epsilon)
        sums_ref[...] = sums * scale
        copy.start()

    block = 2 * lanes
    other = jnp.concatenate([key] * (block // lanes), axis=1)
    bests = []
    for start in range(0, total, block):
        if start == 0 * block:
            centre()
        stop = start + block
        scores = dot(keys, keys[start:stop], ((1,), (1,)))
        allowed = other * side[:, start:stop] > size[:, start:stop]
        bests.append(jnp.max(jnp.where(allowed, scores, -1.0), axis=0, keepdims=True))
    best = jnp.concatenate(bests, axis=1)
    sub = iota((lanes, owners), 0)
    rows = jnp.full((lanes, owners), -1.0, f32)
    for s in range(slots):
        rows = jnp.where(sub == s, best[:, s * owners : (s + 1) * owners], rows)
    rows = rows.T
    shard_count = owners // members
    for m in range(members):
        best_ref[pl.ds(m, shard_count, members), :] = rows[m * shard_count : (m + 1) * shard_count]
    copy.wait()


def exact_dot(values, hot, contract=((1,), (0,))):
    first = values.astype(bf16)
    rest = values - first.astype(f32)
    second = rest.astype(bf16)
    third = (rest - second.astype(f32)).astype(bf16)
    return dot(first, hot, contract) + dot(second, hot, contract) + dot(third, hot, contract)


def unpack_kernel(back_ref, route_ref, out_ref):
    owner = route_ref[0:1, :]
    slot = route_ref[1:2, :]
    back = back_ref[...]
    row_count = owner.shape[1]
    hot = one_hot(iota((back.shape[0], row_count), 0) == owner)
    found = exact_dot(back, hot, ((0,), (0,)))[0:8]
    mine = iota((8, row_count), 0) == slot
    out_ref[...] = jnp.sum(jnp.where(mine, found, 0.0), axis=0, keepdims=True)


def shards(embeddings, clusters, row_ids, owner_map):
    owners = lax.axis_size("shard") * lax.axis_size("member")
    local_rows, width = embeddings.shape
    cluster_count = owner_map.shape[0]
    per_owner = cluster_count // owners
    tiles = pairs * (width // lanes) + 1
    hbm = pl.BlockSpec(memory_space=pltpu.HBM)
    packed, route = pl.pallas_call(
        functools.partial(pack_kernel, members=lax.axis_size("member")),
        in_specs=[hbm] * 4,
        out_shape=(
            jax.ShapeDtypeStruct((owners * tiles, lanes), i32),
            jax.ShapeDtypeStruct((8, local_rows), i32),
        ),
        scratch_shapes=[
            pltpu.VMEM((local_rows, width), f32),
            pltpu.VMEM((1, local_rows), i32),
            pltpu.VMEM((1, local_rows), i32),
            pltpu.VMEM((1, cluster_count), i32),
            pltpu.SemaphoreType.DMA((4,)),
        ],
        compiler_params=params,
        name="pack",
    )(
        *[
            pltpu.with_memory_space_constraint(x, pltpu.HBM)
            for x in (
                embeddings,
                clusters.reshape(1, local_rows),
                row_ids.reshape(1, local_rows),
                owner_map.reshape(1, cluster_count),
            )
        ]
    )
    packed = packed.reshape(owners, tiles, 1, lanes)
    received = lax.all_to_all(packed, exchange, split_axis=0, concat_axis=0, tiled=True)
    received = received.reshape(owners * tiles, lanes)
    centroids, best = pl.pallas_call(
        functools.partial(score_kernel, members=lax.axis_size("member")),
        out_shape=(
            jax.ShapeDtypeStruct((per_owner, width), f32),
            jax.ShapeDtypeStruct((owners, lanes), f32),
        ),
        out_specs=(hbm, pl.BlockSpec(memory_space=pltpu.VMEM)),
        scratch_shapes=[pltpu.VMEM((per_owner, width), f32), pltpu.SemaphoreType.DMA(())],
        compiler_params=params,
        name="score",
    )(received)
    returned = lax.all_to_all(
        best.reshape(owners, 1, lanes), axes, split_axis=0, concat_axis=0, tiled=True
    )
    earlier_max = pl.pallas_call(
        unpack_kernel,
        out_shape=jax.ShapeDtypeStruct((1, local_rows), f32),
        compiler_params=params,
        name="unpack",
    )(returned.reshape(owners, lanes), route)
    return (centroids, earlier_max.reshape(local_rows))


def solution(mesh):
    placed = (P(axes, None), P(axes), P(axes), P())
    return jax.shard_map(
        shards,
        mesh=mesh,
        in_specs=placed,
        out_specs=(P(axes, None), P(axes)),
        check_vma=False,
    )
```

```python
import jax
import jax.numpy as jnp
from jax import lax
from jax.experimental import pallas as pl
from jax.experimental.pallas import tpu as pltpu
from jax.sharding import PartitionSpec as P

epsilon = 1e-06
axes = ("shard", "member")
pairs = 3
slots = 2 * pairs
lanes = 128
id_base = 256
id_range = 32768
full = 32767.0
fields = 16
norm_unit = 256
norm_bytes = 6
f32 = jnp.float32
bf16 = jnp.bfloat16
i32 = jnp.int32
low_half = 0xFFFF
params = pltpu.CompilerParams(vmem_limit_bytes=24 << 20)


def iota(shape, dim):
    return lax.broadcasted_iota(i32, shape, dim)


def dot(a, b, contract=((1,), (0,))):
    return lax.dot_general(a, b, (contract, ((), ())), preferred_element_type=f32)


def one_hot(mask):
    return jnp.where(mask, 1.0, 0.0).astype(bf16)


def count(mask):
    return jnp.sum(jnp.where(mask, 1.0, 0.0), axis=0, keepdims=True)


def to_bytes(values, unit, n):
    digits = []
    rest = values * (1.0 / unit)
    for _ in range(n):
        digit = jnp.floor(rest)
        digits.append(digit)
        rest = (rest - digit) * id_base
    return digits


def pack_kernel(
    rows_hbm,
    clusters_hbm,
    ids_hbm,
    owners_hbm,
    sent_ref,
    route_ref,
    rows_ref,
    clusters_ref,
    ids_ref,
    owners_ref,
    sems,
):
    index_copies = (
        pltpu.make_async_copy(owners_hbm, owners_ref, sems.at[0]),
        pltpu.make_async_copy(clusters_hbm, clusters_ref, sems.at[1]),
        pltpu.make_async_copy(ids_hbm, ids_ref, sems.at[2]),
    )
    copy = pltpu.make_async_copy(rows_hbm, rows_ref, sems.at[3])
    for index_copy in index_copies:
        index_copy.start()
    copy.start()
    for index_copy in index_copies:
        index_copy.wait()
    clusters = clusters_ref[...]
    ids = ids_ref[...]
    owner_map = owners_ref[...].astype(f32)
    row_count, width = rows_ref.shape
    tiles = pairs * (width // lanes) + 1
    owners = sent_ref.shape[0] // tiles
    cluster_count = owner_map.shape[1]

    square = (cluster_count, cluster_count)
    diagonal = iota(square, 0) == iota(square, 1)
    before = iota(square, 0) < iota(square, 1)
    spread = jnp.where(diagonal, owner_map, 0.0).astype(bf16)
    map_col = dot(spread, jnp.ones(square, bf16))
    rank_map = count(before & (map_col == owner_map))
    sub = iota((8, cluster_count), 0)
    table = jnp.where(sub == 0, owner_map, jnp.where(sub == 1, rank_map, 0.0)).astype(bf16)
    cluster_hot = one_hot(iota((cluster_count, row_count), 0) == clusters)
    found = dot(table, cluster_hot)
    owner_col = dot(cluster_hot, map_col[:, :row_count].astype(bf16), ((0,), (0,)))
    slot = count(before & (owner_col == found[0:1])).astype(i32)
    owner = found[0:1].astype(i32)
    rank = found[1:2].astype(i32)

    copy.wait()
    rows = rows_ref[...]
    power = jnp.sum(rows * rows, axis=1, keepdims=True) + epsilon
    inverse = lax.rsqrt(power)
    norm = power * inverse
    largest = jnp.max(jnp.abs(rows), axis=1, keepdims=True) * inverse
    step = jnp.clip(jnp.ceil(largest * full), 1.0, full)
    codes = jnp.floor(rows * (inverse * (full * full / step)) + 0.5)
    upper = codes.astype(bf16)
    halves = jnp.concatenate([upper, (codes - upper.astype(f32)).astype(bf16)], axis=0)
    norm_row = jnp.sum(jnp.where(diagonal, norm, 0.0), axis=0, keepdims=True)
    step_row = jnp.sum(jnp.where(diagonal, step, 0.0), axis=0, keepdims=True)

    side = (2 * rank - 1).astype(f32)
    values = [side * digit for digit in to_bytes((id_range - ids).astype(f32), id_base, 2)]
    values = values + [(rank + 1).astype(f32)]
    values = values + to_bytes(step_row, id_base, 2)
    values = values + to_bytes(norm_row, norm_unit, norm_bytes)
    lane = iota((lanes, row_count), 0)
    field = jnp.where(lane // fields == slot, lane % fields, -1)
    notes = jnp.zeros((lanes, row_count), f32)
    for k, value in enumerate(values):
        notes = jnp.where(field == k, value, notes)
    notes = notes.astype(bf16)

    mine = iota((owners, row_count), 0) == owner
    takes = []
    for s in range(slots):
        take = one_hot(mine & (slot == s))
        takes.append(jnp.concatenate([take, take], axis=1))
    placed = dot(jnp.concatenate(takes, axis=0), halves).astype(i32)
    for p in range(pairs):
        even = placed[2 * p * owners : (2 * p + 1) * owners]
        odd = placed[(2 * p + 1) * owners : (2 * p + 2) * owners]
        words = (odd << 16) | (even & low_half)
        for t in range(width // lanes):
            tile = p * (width // lanes) + t
            sent_ref[pl.ds(tile, owners, tiles), :] = words[:, t * lanes : (t + 1) * lanes]
    words = dot(one_hot(mine), notes, ((1,), (1,))).astype(i32)
    sent_ref[pl.ds(tiles - 1, owners, tiles), :] = words
    sub = iota(route_ref.shape, 0)
    route_ref[...] = jnp.where(sub == 0, owner, slot)


def read_tile(got_ref, tile):
    return got_ref[pl.ds(tile, lanes, got_ref.shape[0] // lanes), :]


def read_notes(got_ref):
    return read_tile(got_ref, got_ref.shape[0] // lanes - 1).astype(f32).astype(bf16)


def read_rows(got_ref, p, steps):
    tiles = (got_ref.shape[0] // lanes - 1) // pairs
    even_step = steps[2 * p] * (1.0 / (65536.0 * full * full))
    odd_step = steps[2 * p + 1] * (1.0 / (full * full))
    even = []
    odd = []
    for t in range(tiles):
        words = read_tile(got_ref, p * tiles + t)
        even.append((words << 16).astype(f32) * even_step)
        odd.append((words >> 16).astype(f32) * odd_step)
    return [jnp.concatenate(even, axis=1), jnp.concatenate(odd, axis=1)]


def along_sublanes(notes, first):
    sub = iota((lanes, lanes), 0)
    field = sub % fields
    weight = jnp.where(field == first, float(id_base), 0.0)
    weight = jnp.where(field == first + 1, 1.0, weight)
    of = sub // fields
    spread = [jnp.where(of == s, weight, 0.0).astype(bf16) for s in range(slots)]
    tall = dot(notes, jnp.concatenate(spread, axis=1))
    return [tall[:, s * lanes : (s + 1) * lanes] for s in range(slots)]


def score_kernel(got_ref, sums_ref, best_ref):
    owners = lanes
    total = slots * owners
    owned, width = sums_ref.shape
    notes = read_notes(got_ref)
    sub = iota((8 * slots, lanes), 0)
    field = iota((8 * slots, lanes), 1) - fields * (sub // 8)
    kind = sub % 8
    pick = jnp.where((kind == 0) & (field == 0), float(id_base), 0.0)
    pick = jnp.where((kind == 0) & (field == 1), 1.0, pick)
    pick = jnp.where((kind == 1) & (field == 2), 1.0, pick)
    for k in range(norm_bytes):
        weight = float(norm_unit) / float(id_base) ** k
        pick = jnp.where((kind == 2) & (field == 5 + k), weight, pick)
    wide = dot(pick.astype(bf16), notes, ((1,), (1,)))
    line = [
        jnp.concatenate([wide[8 * s + k : 8 * s + k + 1] for s in range(slots)], axis=1)
        for k in range(3)
    ]
    side = jnp.where(line[0] > 0.0, 1.0, -1.0)
    size = jnp.abs(line[0])
    key = jnp.concatenate(along_sublanes(notes, 0), axis=0)
    step = along_sublanes(notes, 3)
    exact = []
    for p in range(pairs):
        exact = exact + read_rows(got_ref, p, step)
    exact = jnp.concatenate(exact, axis=0)
    keys = exact.astype(bf16)
    rest = (exact - keys.astype(f32)).astype(bf16)

    def centre():
        sub = iota((8, total), 0)
        coarse = line[2].astype(bf16).astype(f32)
        weight = jnp.where(sub < owned, coarse, line[2] - coarse)
        weight = jnp.where(line[1] == (sub % owned + 1).astype(f32), weight, 0.0)
        weight = jnp.where(sub < 2 * owned, weight, 0.0).astype(bf16)
        sums = dot(weight, keys) + dot(weight, rest)
        sums = sums[0:owned] + sums[owned : 2 * owned]
        scale = lax.rsqrt(jnp.mean(sums * sums, axis=1, keepdims=True) + epsilon)
        sums_ref[...] = sums * scale

    block = 2 * lanes
    other = jnp.concatenate([key] * (block // lanes), axis=1)
    bests = []
    for start in range(0, total, block):
        if start == 1 * block:
            centre()
        stop = start + block
        scores = dot(keys, keys[start:stop], ((1,), (1,)))
        allowed = other * side[:, start:stop] > size[:, start:stop]
        bests.append(jnp.max(jnp.where(allowed, scores, -1.0), axis=0, keepdims=True))
    best = jnp.concatenate(bests, axis=1)
    sub = iota((lanes, owners), 0)
    rows = jnp.full((lanes, owners), -1.0, f32)
    for s in range(slots):
        rows = jnp.where(sub == s, best[:, s * owners : (s + 1) * owners], rows)
    best_ref[...] = rows.T


def exact_dot(values, hot, contract=((1,), (0,))):
    first = values.astype(bf16)
    rest = values - first.astype(f32)
    second = rest.astype(bf16)
    third = (rest - second.astype(f32)).astype(bf16)
    return dot(first, hot, contract) + dot(second, hot, contract) + dot(third, hot, contract)


def unpack_kernel(back_ref, route_ref, sums_ref, centres_ref, out_ref):
    centres_ref[...] = sums_ref[...]
    owner = route_ref[0:1, :]
    slot = route_ref[1:2, :]
    back = back_ref[...]
    row_count = owner.shape[1]
    hot = one_hot(iota((back.shape[0], row_count), 0) == owner)
    found = exact_dot(back, hot, ((0,), (0,)))[0:8]
    mine = iota((8, row_count), 0) == slot
    out_ref[...] = jnp.sum(jnp.where(mine, found, 0.0), axis=0, keepdims=True)


def shards(embeddings, clusters, row_ids, owner_map):
    owners = lax.axis_size("shard") * lax.axis_size("member")
    local_rows, width = embeddings.shape
    cluster_count = owner_map.shape[0]
    per_owner = cluster_count // owners
    tiles = pairs * (width // lanes) + 1
    hbm = pl.BlockSpec(memory_space=pltpu.HBM)
    packed, route = pl.pallas_call(
        pack_kernel,
        in_specs=[hbm] * 4,
        out_shape=(
            jax.ShapeDtypeStruct((owners * tiles, lanes), i32),
            jax.ShapeDtypeStruct((8, local_rows), i32),
        ),
        scratch_shapes=[
            pltpu.VMEM((local_rows, width), f32),
            pltpu.VMEM((1, local_rows), i32),
            pltpu.VMEM((1, local_rows), i32),
            pltpu.VMEM((1, cluster_count), i32),
            pltpu.SemaphoreType.DMA((4,)),
        ],
        compiler_params=params,
        name="pack",
    )(
        *[
            pltpu.with_memory_space_constraint(x, pltpu.HBM)
            for x in (
                embeddings,
                clusters.reshape(1, local_rows),
                row_ids.reshape(1, local_rows),
                owner_map.reshape(1, cluster_count),
            )
        ]
    )
    packed = packed.reshape(owners, tiles, 1, lanes)
    received = lax.all_to_all(packed, axes, split_axis=0, concat_axis=0, tiled=True)
    received = received.reshape(owners * tiles, lanes)
    centroids, best = pl.pallas_call(
        score_kernel,
        out_shape=(
            jax.ShapeDtypeStruct((per_owner, width), f32),
            jax.ShapeDtypeStruct((owners, lanes), f32),
        ),
        compiler_params=params,
        name="score",
    )(received)
    returned = lax.all_to_all(
        best.reshape(owners, 1, lanes), axes, split_axis=0, concat_axis=0, tiled=True
    )
    centroids, earlier_max = pl.pallas_call(
        unpack_kernel,
        out_shape=(
            jax.ShapeDtypeStruct((per_owner, width), f32),
            jax.ShapeDtypeStruct((1, local_rows), f32),
        ),
        compiler_params=params,
        name="unpack",
    )(returned.reshape(owners, lanes), route, centroids)
    return (centroids, earlier_max.reshape(local_rows))


def solution(mesh):
    placed = (P(axes, None), P(axes), P(axes), P())
    return jax.shard_map(
        shards,
        mesh=mesh,
        in_specs=placed,
        out_specs=(P(axes, None), P(axes)),
        check_vma=False,
    )
```

```python
import jax
import jax.numpy as jnp
from jax import lax
from jax.experimental import pallas as pl
from jax.experimental.pallas import tpu as pltpu
from jax.sharding import PartitionSpec as P

epsilon = 1e-06
axes = ("shard", "member")
pairs = 3
slots = 2 * pairs
lanes = 128
id_base = 256
id_range = 32768
full = 32767.0
fields = 16
norm_unit = 256
norm_bytes = 6
f32 = jnp.float32
bf16 = jnp.bfloat16
i32 = jnp.int32
low_half = 0xFFFF
params = pltpu.CompilerParams(vmem_limit_bytes=24 << 20)


def iota(shape, dim):
    return lax.broadcasted_iota(i32, shape, dim)


def dot(a, b, contract=((1,), (0,))):
    return lax.dot_general(a, b, (contract, ((), ())), preferred_element_type=f32)


def one_hot(mask):
    return jnp.where(mask, 1.0, 0.0).astype(bf16)


def count(mask):
    return jnp.sum(jnp.where(mask, 1.0, 0.0), axis=0, keepdims=True)


def to_bytes(values, unit, n):
    digits = []
    rest = values * (1.0 / unit)
    for _ in range(n):
        digit = jnp.floor(rest)
        digits.append(digit)
        rest = (rest - digit) * id_base
    return digits


def pack_kernel(
    rows_hbm,
    clusters_hbm,
    ids_hbm,
    owners_hbm,
    sent_ref,
    route_ref,
    rows_ref,
    clusters_ref,
    ids_ref,
    owners_ref,
    sems,
):
    index_copies = (
        pltpu.make_async_copy(owners_hbm, owners_ref, sems.at[0]),
        pltpu.make_async_copy(clusters_hbm, clusters_ref, sems.at[1]),
        pltpu.make_async_copy(ids_hbm, ids_ref, sems.at[2]),
    )
    copy = pltpu.make_async_copy(rows_hbm, rows_ref, sems.at[3])
    for index_copy in index_copies:
        index_copy.start()
    copy.start()
    for index_copy in index_copies:
        index_copy.wait()
    clusters = clusters_ref[...]
    ids = ids_ref[...]
    owner_map = owners_ref[...].astype(f32)
    row_count, width = rows_ref.shape
    tiles = pairs * (width // lanes) + 1
    owners = sent_ref.shape[0] // tiles
    cluster_count = owner_map.shape[1]

    square = (cluster_count, cluster_count)
    diagonal = iota(square, 0) == iota(square, 1)
    before = iota(square, 0) < iota(square, 1)
    spread = jnp.where(diagonal, owner_map, 0.0).astype(bf16)
    map_col = dot(spread, jnp.ones(square, bf16))
    rank_map = count(before & (map_col == owner_map))
    sub = iota((8, cluster_count), 0)
    table = jnp.where(sub == 0, owner_map, jnp.where(sub == 1, rank_map, 0.0)).astype(bf16)
    cluster_hot = one_hot(iota((cluster_count, row_count), 0) == clusters)
    found = dot(table, cluster_hot)
    owner_col = dot(cluster_hot, map_col[:, :row_count].astype(bf16), ((0,), (0,)))
    slot = count(before & (owner_col == found[0:1])).astype(i32)
    owner = found[0:1].astype(i32)
    rank = found[1:2].astype(i32)

    copy.wait()
    rows = rows_ref[...]
    power = jnp.sum(rows * rows, axis=1, keepdims=True) + epsilon
    inverse = lax.rsqrt(power)
    norm = power * inverse
    largest = jnp.max(jnp.abs(rows), axis=1, keepdims=True) * inverse
    step = jnp.clip(jnp.ceil(largest * full), 1.0, full)
    codes = jnp.floor(rows * (inverse * (full * full / step)) + 0.5)
    wanted = (rows * inverse).astype(bf16).astype(f32)
    reached = (codes * (step * (1.0 / (full * full)))).astype(bf16).astype(f32)
    missing = wanted - reached
    least = step * (0.9 / (full * full))
    codes = codes + jnp.where(missing >= least, 1.0, jnp.where(missing <= -least, -1.0, 0.0))
    codes = jnp.clip(codes, -full, full)
    upper = codes.astype(bf16)
    halves = jnp.concatenate([upper, (codes - upper.astype(f32)).astype(bf16)], axis=0)
    norm_row = jnp.sum(jnp.where(diagonal, norm, 0.0), axis=0, keepdims=True)
    step_row = jnp.sum(jnp.where(diagonal, step, 0.0), axis=0, keepdims=True)

    side = (2 * rank - 1).astype(f32)
    values = [side * digit for digit in to_bytes((id_range - ids).astype(f32), id_base, 2)]
    values = values + [(rank + 1).astype(f32)]
    values = values + to_bytes(step_row, id_base, 2)
    values = values + to_bytes(norm_row, norm_unit, norm_bytes)
    lane = iota((lanes, row_count), 0)
    field = jnp.where(lane // fields == slot, lane % fields, -1)
    notes = jnp.zeros((lanes, row_count), f32)
    for k, value in enumerate(values):
        notes = jnp.where(field == k, value, notes)
    notes = notes.astype(bf16)

    mine = iota((owners, row_count), 0) == owner
    takes = []
    for s in range(slots):
        take = one_hot(mine & (slot == s))
        takes.append(jnp.concatenate([take, take], axis=1))
    placed = dot(jnp.concatenate(takes, axis=0), halves).astype(i32)
    for p in range(pairs):
        even = placed[2 * p * owners : (2 * p + 1) * owners]
        odd = placed[(2 * p + 1) * owners : (2 * p + 2) * owners]
        words = (odd << 16) | (even & low_half)
        for t in range(width // lanes):
            tile = p * (width // lanes) + t
            sent_ref[pl.ds(tile, owners, tiles), :] = words[:, t * lanes : (t + 1) * lanes]
    words = dot(one_hot(mine), notes, ((1,), (1,))).astype(i32)
    sent_ref[pl.ds(tiles - 1, owners, tiles), :] = words
    sub = iota(route_ref.shape, 0)
    route_ref[...] = jnp.where(sub == 0, owner, slot)


def read_tile(got_ref, tile):
    return got_ref[pl.ds(tile, lanes, got_ref.shape[0] // lanes), :]


def read_notes(got_ref):
    return read_tile(got_ref, got_ref.shape[0] // lanes - 1).astype(f32).astype(bf16)


def read_rows(got_ref, p, steps):
    tiles = (got_ref.shape[0] // lanes - 1) // pairs
    even_step = steps[2 * p] * (1.0 / (65536.0 * full * full))
    odd_step = steps[2 * p + 1] * (1.0 / (full * full))
    even = []
    odd = []
    for t in range(tiles):
        words = read_tile(got_ref, p * tiles + t)
        even.append((words << 16).astype(f32) * even_step)
        odd.append((words >> 16).astype(f32) * odd_step)
    return [jnp.concatenate(even, axis=1), jnp.concatenate(odd, axis=1)]


def along_sublanes(notes, first):
    sub = iota((lanes, lanes), 0)
    field = sub % fields
    weight = jnp.where(field == first, float(id_base), 0.0)
    weight = jnp.where(field == first + 1, 1.0, weight)
    of = sub // fields
    spread = [jnp.where(of == s, weight, 0.0).astype(bf16) for s in range(slots)]
    tall = dot(notes, jnp.concatenate(spread, axis=1))
    return [tall[:, s * lanes : (s + 1) * lanes] for s in range(slots)]


def score_kernel(got_ref, sums_ref, best_ref):
    owners = lanes
    total = slots * owners
    owned, width = sums_ref.shape
    notes = read_notes(got_ref)
    sub = iota((8 * slots, lanes), 0)
    field = iota((8 * slots, lanes), 1) - fields * (sub // 8)
    kind = sub % 8
    pick = jnp.where((kind == 0) & (field == 0), float(id_base), 0.0)
    pick = jnp.where((kind == 0) & (field == 1), 1.0, pick)
    pick = jnp.where((kind == 1) & (field == 2), 1.0, pick)
    for k in range(norm_bytes):
        weight = float(norm_unit) / float(id_base) ** k
        pick = jnp.where((kind == 2) & (field == 5 + k), weight, pick)
    wide = dot(pick.astype(bf16), notes, ((1,), (1,)))
    line = [
        jnp.concatenate([wide[8 * s + k : 8 * s + k + 1] for s in range(slots)], axis=1)
        for k in range(3)
    ]
    side = jnp.where(line[0] > 0.0, 1.0, -1.0)
    size = jnp.abs(line[0])
    key = jnp.concatenate(along_sublanes(notes, 0), axis=0)
    step = along_sublanes(notes, 3)
    exact = []
    for p in range(pairs):
        exact = exact + read_rows(got_ref, p, step)
    exact = jnp.concatenate(exact, axis=0)
    keys = exact.astype(bf16)
    rest = (exact - keys.astype(f32)).astype(bf16)

    def centre():
        sub = iota((8, total), 0)
        coarse = line[2].astype(bf16).astype(f32)
        weight = jnp.where(sub < owned, coarse, line[2] - coarse)
        weight = jnp.where(line[1] == (sub % owned + 1).astype(f32), weight, 0.0)
        weight = jnp.where(sub < 2 * owned, weight, 0.0).astype(bf16)
        sums = dot(weight, keys) + dot(weight, rest)
        sums = sums[0:owned] + sums[owned : 2 * owned]
        scale = lax.rsqrt(jnp.mean(sums * sums, axis=1, keepdims=True) + epsilon)
        sums_ref[...] = sums * scale

    block = 2 * lanes
    other = jnp.concatenate([key] * (block // lanes), axis=1)
    bests = []
    for start in range(0, total, block):
        if start == 1 * block:
            centre()
        stop = start + block
        scores = dot(keys, keys[start:stop], ((1,), (1,)))
        allowed = other * side[:, start:stop] > size[:, start:stop]
        bests.append(jnp.max(jnp.where(allowed, scores, -1.0), axis=0, keepdims=True))
    best = jnp.concatenate(bests, axis=1)
    sub = iota((lanes, owners), 0)
    rows = jnp.full((lanes, owners), -1.0, f32)
    for s in range(slots):
        rows = jnp.where(sub == s, best[:, s * owners : (s + 1) * owners], rows)
    best_ref[...] = rows.T


def exact_dot(values, hot, contract=((1,), (0,))):
    first = values.astype(bf16)
    rest = values - first.astype(f32)
    second = rest.astype(bf16)
    third = (rest - second.astype(f32)).astype(bf16)
    return dot(first, hot, contract) + dot(second, hot, contract) + dot(third, hot, contract)


def unpack_kernel(back_ref, route_ref, sums_ref, centres_ref, out_ref):
    centres_ref[...] = sums_ref[...]
    owner = route_ref[0:1, :]
    slot = route_ref[1:2, :]
    back = back_ref[...]
    row_count = owner.shape[1]
    hot = one_hot(iota((back.shape[0], row_count), 0) == owner)
    found = exact_dot(back, hot, ((0,), (0,)))[0:8]
    mine = iota((8, row_count), 0) == slot
    out_ref[...] = jnp.sum(jnp.where(mine, found, 0.0), axis=0, keepdims=True)


def shards(embeddings, clusters, row_ids, owner_map):
    owners = lax.axis_size("shard") * lax.axis_size("member")
    local_rows, width = embeddings.shape
    cluster_count = owner_map.shape[0]
    per_owner = cluster_count // owners
    tiles = pairs * (width // lanes) + 1
    hbm = pl.BlockSpec(memory_space=pltpu.HBM)
    packed, route = pl.pallas_call(
        pack_kernel,
        in_specs=[hbm] * 4,
        out_shape=(
            jax.ShapeDtypeStruct((owners * tiles, lanes), i32),
            jax.ShapeDtypeStruct((8, local_rows), i32),
        ),
        scratch_shapes=[
            pltpu.VMEM((local_rows, width), f32),
            pltpu.VMEM((1, local_rows), i32),
            pltpu.VMEM((1, local_rows), i32),
            pltpu.VMEM((1, cluster_count), i32),
            pltpu.SemaphoreType.DMA((4,)),
        ],
        compiler_params=params,
        name="pack",
    )(
        *[
            pltpu.with_memory_space_constraint(x, pltpu.HBM)
            for x in (
                embeddings,
                clusters.reshape(1, local_rows),
                row_ids.reshape(1, local_rows),
                owner_map.reshape(1, cluster_count),
            )
        ]
    )
    packed = packed.reshape(owners, tiles, 1, lanes)
    received = lax.all_to_all(packed, axes, split_axis=0, concat_axis=0, tiled=True)
    received = received.reshape(owners * tiles, lanes)
    centroids, best = pl.pallas_call(
        score_kernel,
        out_shape=(
            jax.ShapeDtypeStruct((per_owner, width), f32),
            jax.ShapeDtypeStruct((owners, lanes), f32),
        ),
        compiler_params=params,
        name="score",
    )(received)
    returned = lax.all_to_all(
        best.reshape(owners, 1, lanes), axes, split_axis=0, concat_axis=0, tiled=True
    )
    centroids, earlier_max = pl.pallas_call(
        unpack_kernel,
        out_shape=(
            jax.ShapeDtypeStruct((per_owner, width), f32),
            jax.ShapeDtypeStruct((1, local_rows), f32),
        ),
        compiler_params=params,
        name="unpack",
    )(returned.reshape(owners, lanes), route, centroids)
    return (centroids, earlier_max.reshape(local_rows))


def solution(mesh):
    placed = (P(axes, None), P(axes), P(axes), P())
    return jax.shard_map(
        shards,
        mesh=mesh,
        in_specs=placed,
        out_specs=(P(axes, None), P(axes)),
        check_vma=False,
    )
```

```python
import jax
import jax.numpy as jnp
from jax import lax
from jax.experimental import pallas as pl
from jax.experimental.pallas import tpu as pltpu
from jax.sharding import PartitionSpec as P

epsilon = 1e-06
axes = ("shard", "member")
pairs = 3
slots = 2 * pairs
lanes = 128
id_base = 256
id_range = 32768
full = 32767.0
fields = 16
norm_unit = 256
norm_bytes = 6
f32 = jnp.float32
bf16 = jnp.bfloat16
i32 = jnp.int32
low_half = 0xFFFF
params = pltpu.CompilerParams(vmem_limit_bytes=24 << 20)


def iota(shape, dim):
    return lax.broadcasted_iota(i32, shape, dim)


def dot(a, b, contract=((1,), (0,))):
    return lax.dot_general(a, b, (contract, ((), ())), preferred_element_type=f32)


def one_hot(mask):
    return jnp.where(mask, 1.0, 0.0).astype(bf16)


def count(mask):
    return jnp.sum(jnp.where(mask, 1.0, 0.0), axis=0, keepdims=True)


def to_bytes(values, unit, n):
    digits = []
    rest = values * (1.0 / unit)
    for _ in range(n):
        digit = jnp.floor(rest)
        digits.append(digit)
        rest = (rest - digit) * id_base
    return digits


def pack_kernel(
    rows_hbm,
    clusters_hbm,
    ids_hbm,
    owners_hbm,
    sent_ref,
    route_ref,
    rows_ref,
    clusters_ref,
    ids_ref,
    owners_ref,
    sems,
):
    index_copies = (
        pltpu.make_async_copy(owners_hbm, owners_ref, sems.at[0]),
        pltpu.make_async_copy(clusters_hbm, clusters_ref, sems.at[1]),
        pltpu.make_async_copy(ids_hbm, ids_ref, sems.at[2]),
    )
    copy = pltpu.make_async_copy(rows_hbm, rows_ref, sems.at[3])
    for index_copy in index_copies:
        index_copy.start()
    copy.start()
    for index_copy in index_copies:
        index_copy.wait()
    copy.wait()
    clusters = clusters_ref[...]
    ids = ids_ref[...]
    owner_map = owners_ref[...].astype(f32)
    row_count, width = rows_ref.shape
    tiles = pairs * (width // lanes) + 1
    owners = sent_ref.shape[0] // tiles
    cluster_count = owner_map.shape[1]

    square = (cluster_count, cluster_count)
    diagonal = iota(square, 0) == iota(square, 1)
    before = iota(square, 0) < iota(square, 1)
    spread = jnp.where(diagonal, owner_map, 0.0).astype(bf16)
    map_col = dot(spread, jnp.ones(square, bf16))
    rank_map = count(before & (map_col == owner_map))
    sub = iota((8, cluster_count), 0)
    table = jnp.where(sub == 0, owner_map, jnp.where(sub == 1, rank_map, 0.0)).astype(bf16)
    cluster_hot = one_hot(iota((cluster_count, row_count), 0) == clusters)
    found = dot(table, cluster_hot)
    owner_col = dot(cluster_hot, map_col[:, :row_count].astype(bf16), ((0,), (0,)))
    slot = count(before & (owner_col == found[0:1])).astype(i32)
    owner = found[0:1].astype(i32)
    rank = found[1:2].astype(i32)

    rows = rows_ref[...]
    power = jnp.sum(rows * rows, axis=1, keepdims=True) + epsilon
    inverse = lax.rsqrt(power)
    norm = power * inverse
    largest = jnp.max(jnp.abs(rows), axis=1, keepdims=True) * inverse
    step = jnp.clip(jnp.ceil(largest * full), 1.0, full)
    codes = jnp.floor(rows * (inverse * (full * full / step)) + 0.5)
    upper = codes.astype(bf16)
    halves = jnp.concatenate([upper, (codes - upper.astype(f32)).astype(bf16)], axis=0)
    norm_row = jnp.sum(jnp.where(diagonal, norm, 0.0), axis=0, keepdims=True)
    step_row = jnp.sum(jnp.where(diagonal, step, 0.0), axis=0, keepdims=True)

    side = (2 * rank - 1).astype(f32)
    values = [side * digit for digit in to_bytes((id_range - ids).astype(f32), id_base, 2)]
    values = values + [(rank + 1).astype(f32)]
    values = values + to_bytes(step_row, id_base, 2)
    values = values + to_bytes(norm_row, norm_unit, norm_bytes)
    lane = iota((lanes, row_count), 0)
    field = jnp.where(lane // fields == slot, lane % fields, -1)
    notes = jnp.zeros((lanes, row_count), f32)
    for k, value in enumerate(values):
        notes = jnp.where(field == k, value, notes)
    notes = notes.astype(bf16)

    mine = iota((owners, row_count), 0) == owner
    takes = []
    for s in range(slots):
        take = one_hot(mine & (slot == s))
        takes.append(jnp.concatenate([take, take], axis=1))
    placed = dot(jnp.concatenate(takes, axis=0), halves).astype(i32)
    for p in range(pairs):
        even = placed[2 * p * owners : (2 * p + 1) * owners]
        odd = placed[(2 * p + 1) * owners : (2 * p + 2) * owners]
        words = (odd << 16) | (even & low_half)
        for t in range(width // lanes):
            tile = p * (width // lanes) + t
            sent_ref[pl.ds(tile, owners, tiles), :] = words[:, t * lanes : (t + 1) * lanes]
    words = dot(one_hot(mine), notes, ((1,), (1,))).astype(i32)
    sent_ref[pl.ds(tiles - 1, owners, tiles), :] = words
    sub = iota(route_ref.shape, 0)
    route_ref[...] = jnp.where(sub == 0, owner, slot)


def read_tile(got_ref, tile):
    return got_ref[pl.ds(tile, lanes, got_ref.shape[0] // lanes), :]


def read_notes(got_ref):
    return read_tile(got_ref, got_ref.shape[0] // lanes - 1).astype(f32).astype(bf16)


def read_rows(got_ref, p, steps):
    tiles = (got_ref.shape[0] // lanes - 1) // pairs
    even_step = steps[2 * p] * (1.0 / (65536.0 * full * full))
    odd_step = steps[2 * p + 1] * (1.0 / (full * full))
    even = []
    odd = []
    for t in range(tiles):
        words = read_tile(got_ref, p * tiles + t)
        even.append((words << 16).astype(f32) * even_step)
        odd.append((words >> 16).astype(f32) * odd_step)
    return [jnp.concatenate(even, axis=1), jnp.concatenate(odd, axis=1)]


def along_sublanes(notes, first):
    sub = iota((lanes, lanes), 0)
    field = sub % fields
    weight = jnp.where(field == first, float(id_base), 0.0)
    weight = jnp.where(field == first + 1, 1.0, weight)
    of = sub // fields
    spread = [jnp.where(of == s, weight, 0.0).astype(bf16) for s in range(slots)]
    tall = dot(notes, jnp.concatenate(spread, axis=1))
    return [tall[:, s * lanes : (s + 1) * lanes] for s in range(slots)]


def score_kernel(got_ref, sums_ref, best_ref):
    owners = lanes
    total = slots * owners
    owned, width = sums_ref.shape
    notes = read_notes(got_ref)
    sub = iota((8 * slots, lanes), 0)
    field = iota((8 * slots, lanes), 1) - fields * (sub // 8)
    kind = sub % 8
    pick = jnp.where((kind == 0) & (field == 0), float(id_base), 0.0)
    pick = jnp.where((kind == 0) & (field == 1), 1.0, pick)
    pick = jnp.where((kind == 1) & (field == 2), 1.0, pick)
    for k in range(norm_bytes):
        weight = float(norm_unit) / float(id_base) ** k
        pick = jnp.where((kind == 2) & (field == 5 + k), weight, pick)
    wide = dot(pick.astype(bf16), notes, ((1,), (1,)))
    line = [
        jnp.concatenate([wide[8 * s + k : 8 * s + k + 1] for s in range(slots)], axis=1)
        for k in range(3)
    ]
    side = jnp.where(line[0] > 0.0, 1.0, -1.0)
    size = jnp.abs(line[0])
    key = jnp.concatenate(along_sublanes(notes, 0), axis=0)
    step = along_sublanes(notes, 3)
    exact = []
    for p in range(pairs):
        exact = exact + read_rows(got_ref, p, step)
    exact = jnp.concatenate(exact, axis=0)
    keys = exact.astype(bf16)
    rest = (exact - keys.astype(f32)).astype(bf16)

    def centre():
        sub = iota((8, total), 0)
        coarse = line[2].astype(bf16).astype(f32)
        weight = jnp.where(sub < owned, coarse, line[2] - coarse)
        weight = jnp.where(line[1] == (sub % owned + 1).astype(f32), weight, 0.0)
        weight = jnp.where(sub < 2 * owned, weight, 0.0).astype(bf16)
        sums = dot(weight, keys) + dot(weight, rest)
        sums = sums[0:owned] + sums[owned : 2 * owned]
        scale = lax.rsqrt(jnp.mean(sums * sums, axis=1, keepdims=True) + epsilon)
        sums_ref[...] = sums * scale

    block = 2 * lanes
    other = jnp.concatenate([key] * (block // lanes), axis=1)
    bests = []
    for start in range(0, total, block):
        if start == 1 * block:
            centre()
        stop = start + block
        scores = dot(keys, keys[start:stop], ((1,), (1,)))
        allowed = other * side[:, start:stop] > size[:, start:stop]
        bests.append(jnp.max(jnp.where(allowed, scores, -1.0), axis=0, keepdims=True))
    best = jnp.concatenate(bests, axis=1)
    sub = iota((lanes, owners), 0)
    rows = jnp.full((lanes, owners), -1.0, f32)
    for s in range(slots):
        rows = jnp.where(sub == s, best[:, s * owners : (s + 1) * owners], rows)
    best_ref[...] = rows.T


def exact_dot(values, hot, contract=((1,), (0,))):
    first = values.astype(bf16)
    rest = values - first.astype(f32)
    second = rest.astype(bf16)
    third = (rest - second.astype(f32)).astype(bf16)
    return dot(first, hot, contract) + dot(second, hot, contract) + dot(third, hot, contract)


def unpack_kernel(back_ref, route_ref, sums_ref, centres_ref, out_ref):
    centres_ref[...] = sums_ref[...]
    owner = route_ref[0:1, :]
    slot = route_ref[1:2, :]
    back = back_ref[...]
    row_count = owner.shape[1]
    hot = one_hot(iota((back.shape[0], row_count), 0) == owner)
    found = exact_dot(back, hot, ((0,), (0,)))[0:8]
    mine = iota((8, row_count), 0) == slot
    out_ref[...] = jnp.sum(jnp.where(mine, found, 0.0), axis=0, keepdims=True)


def shards(embeddings, clusters, row_ids, owner_map):
    owners = lax.axis_size("shard") * lax.axis_size("member")
    local_rows, width = embeddings.shape
    cluster_count = owner_map.shape[0]
    per_owner = cluster_count // owners
    tiles = pairs * (width // lanes) + 1
    hbm = pl.BlockSpec(memory_space=pltpu.HBM)
    packed, route = pl.pallas_call(
        pack_kernel,
        in_specs=[hbm] * 4,
        out_shape=(
            jax.ShapeDtypeStruct((owners * tiles, lanes), i32),
            jax.ShapeDtypeStruct((8, local_rows), i32),
        ),
        scratch_shapes=[
            pltpu.VMEM((local_rows, width), f32),
            pltpu.VMEM((1, local_rows), i32),
            pltpu.VMEM((1, local_rows), i32),
            pltpu.VMEM((1, cluster_count), i32),
            pltpu.SemaphoreType.DMA((4,)),
        ],
        compiler_params=params,
        name="pack",
    )(
        *[
            pltpu.with_memory_space_constraint(x, pltpu.HBM)
            for x in (
                embeddings,
                clusters.reshape(1, local_rows),
                row_ids.reshape(1, local_rows),
                owner_map.reshape(1, cluster_count),
            )
        ]
    )
    packed = packed.reshape(owners, tiles, 1, lanes)
    received = lax.all_to_all(packed, axes, split_axis=0, concat_axis=0, tiled=True)
    received = received.reshape(owners * tiles, lanes)
    centroids, best = pl.pallas_call(
        score_kernel,
        out_shape=(
            jax.ShapeDtypeStruct((per_owner, width), f32),
            jax.ShapeDtypeStruct((owners, lanes), f32),
        ),
        compiler_params=params,
        name="score",
    )(received)
    returned = lax.all_to_all(
        best.reshape(owners, 1, lanes), axes, split_axis=0, concat_axis=0, tiled=True
    )
    centroids, earlier_max = pl.pallas_call(
        unpack_kernel,
        out_shape=(
            jax.ShapeDtypeStruct((per_owner, width), f32),
            jax.ShapeDtypeStruct((1, local_rows), f32),
        ),
        compiler_params=params,
        name="unpack",
    )(returned.reshape(owners, lanes), route, centroids)
    return (centroids, earlier_max.reshape(local_rows))


def solution(mesh):
    placed = (P(axes, None), P(axes), P(axes), P())
    return jax.shard_map(
        shards,
        mesh=mesh,
        in_specs=placed,
        out_specs=(P(axes, None), P(axes)),
        check_vma=False,
    )
```
